32 devices in a mesh: panel: 16 (over z, y, x), lag: 2 (over core).
Axes of the slice: x: 2, y: 2, z: 4, core: 2. Of those that a mesh axis runs over, the one named last changes fastest.
Arguments:
- history: bfloat16 [2, 32, 512, 128], P('lag', 'panel'), may hold values from -6 to 6
- weights: bfloat16 [16, 2, 6, 512, 512], P('panel', 'lag'), may hold values from -0.25 to 0.25
- pairs: int32 [16, 2, 6, 3], P('panel', 'lag'), may hold values from 0 to 4, as said below
- counts: int32 [16, 2], P('panel', 'lag'), may hold values from 3 to 6, as said below
- send_list: int32 [16, 2, 5, 2], P(None, 'lag'), may hold values from 0 to 1
- incident: bfloat16 [32, 512, 128], P(('panel', 'lag')), may hold values from -6 to 6
- near_inverse: bfloat16 [32, 512, 512], P(('panel', 'lag')), may hold values from -0.25 to 0.25
Outputs:
- density: bfloat16 [32, 512, 128], P(('panel', 'lag'))
The draws below stay inside these ranges and needn't reach their ends.
Inputs may be any that keep to these rules, and one draw needn't show every extreme that they name: pairs[p, g, k] = (o, c, r) with o in 0 to 4, c in 0 to 1, r in 0 to 1; the (o, c) of one device's pairs are distinct. `counts`: panel index 0 at lag index 0 has 6 pairs.
All inputs are finite; a program needn't handle non-finite values.
Results may differ from the reference program's by a relative error of at most 0.0083.
Values may be sent and summed in bfloat16 or wider, within the bound.
A program may use at most 64 MiB of HBM per device.

```python
import jax
import jax.numpy as jnp
from jax import lax

PB = 512
RHS = 128
PAIRS_DEV = 6
REACH = 2
CAP = 2
BLK_DEV = 2
LAGS = 2
NBLK = 32
N_PANEL = 16


def draw_pairs(key, part):
    offsets = 2 * REACH + 1
    scores = jax.random.randint(jax.random.fold_in(key, 11), (N_PANEL, LAGS, offsets), 0, 1 << 20) * offsets + jnp.arange(offsets, dtype=jnp.int32)
    order = jnp.argsort(scores, axis=-1, stable=True).astype(jnp.int32)
    position = jnp.arange(PAIRS_DEV, dtype=jnp.int32)
    chosen = jnp.take(order, position // CAP, axis=2)
    slot_index = jnp.broadcast_to(position % CAP, (N_PANEL, LAGS, PAIRS_DEV)).astype(jnp.int32)
    reader = jax.random.randint(jax.random.fold_in(key, 12), (N_PANEL, LAGS, PAIRS_DEV), 0, BLK_DEV).astype(jnp.int32)
    return jnp.stack([chosen, slot_index, reader], axis=-1).astype(jnp.int32)


def draw_counts(key, part):
    extra = jax.random.randint(jax.random.fold_in(key, 21), (N_PANEL, LAGS), 0, 4)
    active = jnp.minimum(3 + extra, PAIRS_DEV)
    return active.at[0, 0].set(PAIRS_DEV).astype(jnp.int32)


def with_ends(values, own_key, smallest, high):
    longest = values.shape.index(max(values.shape))
    spots = []
    for shift in (0, 1):
        where = [jax.random.randint(jax.random.fold_in(own_key, axis), (), 0, length) for axis, length in enumerate(values.shape)]
        where[longest] = (where[longest] + shift) % values.shape[longest]
        spots.append(tuple(where))
    return values.at[spots[0]].set(smallest).at[spots[1]].set(high)


def levels(own_key, dims, pieces, least, high):
    loudness = 1.0
    for axis_at, blocks in pieces:
        heights = jax.random.uniform(jax.random.fold_in(jax.random.fold_in(own_key, 6), axis_at), (blocks,), jnp.float32, least / len(pieces), high / len(pieces))
        loudness = loudness * jnp.repeat(jnp.exp(heights), dims[axis_at] // blocks).reshape((-1,) + (1,) * (len(dims) - 1 - axis_at))
    return loudness


def centred(own_key, shape, scale, limit, split=(), kind=jnp.bfloat16):
    gain = levels(own_key, shape, split, -0.22, 0.18) if split else 1.0
    entries = jax.random.normal(own_key, shape, jnp.float32) * scale * gain
    return jnp.minimum(jnp.maximum(entries, -limit), limit).astype(kind)


def setup_inputs(seed: int = 0) -> dict:
    key_list = jax.random.split(jax.random.key(seed), 8)
    history = centred(key_list[0], (LAGS, NBLK, PB, RHS), 1.0, 6.0, ((0, 2), (1, 16)))
    weights = centred(key_list[1], (N_PANEL, LAGS, PAIRS_DEV, PB, PB), PB ** -0.5, 0.25, ((0, 16), (1, 2)))
    pairs = draw_pairs(jax.random.fold_in(key_list[7], 71), 0)
    counts = draw_counts(jax.random.fold_in(key_list[7], 71), 0)
    send_list = with_ends(jax.random.randint(key_list[4], (N_PANEL, LAGS, 2 * REACH + 1, CAP), 0, BLK_DEV), jax.random.fold_in(key_list[4], 1), 0, BLK_DEV - 1).astype(jnp.int32)
    incident = centred(key_list[5], (NBLK, PB, RHS), 1.0, 6.0, ((0, 32),))
    near_inverse = centred(key_list[6], (NBLK, PB, PB), PB ** -0.5, 0.25, ((0, 32),))
    return dict(history=history, weights=weights, pairs=pairs, counts=counts, send_list=send_list, incident=incident, near_inverse=near_inverse)


def reference(history, weights, pairs, counts, send_list, incident, near_inverse):
    summed = jnp.zeros((NBLK, PB, RHS), jnp.float32)

    def per_device(device, summed):
        panel_idx = (device // LAGS).astype(jnp.int32)
        lag_idx = (device % LAGS).astype(jnp.int32)

        def add_pair(pair_index, summed):
            offset = pairs[panel_idx, lag_idx, pair_index, 0]
            slot_index = pairs[panel_idx, lag_idx, pair_index, 1]
            reader = pairs[panel_idx, lag_idx, pair_index, 2]
            source_panel = ((panel_idx + offset - REACH) % N_PANEL).astype(jnp.int32)
            local_block = send_list[source_panel, lag_idx, offset, slot_index]
            source = history[lag_idx, source_panel * BLK_DEV + local_block]
            product = jnp.dot(weights[panel_idx, lag_idx, pair_index], source, preferred_element_type=jnp.float32)
            target = (panel_idx * BLK_DEV + reader).astype(jnp.int32)
            current = lax.dynamic_index_in_dim(summed, target, 0, keepdims=False)
            return lax.dynamic_update_index_in_dim(summed, current + product, target, 0)

        return lax.fori_loop(0, counts[panel_idx, lag_idx], add_pair, summed)

    summed = lax.fori_loop(0, N_PANEL * LAGS, per_device, summed)
    remainder = (incident.astype(jnp.float32) - summed).astype(jnp.bfloat16)
    density = jnp.einsum("bij,bjr->bir", near_inverse.astype(jnp.float32), remainder.astype(jnp.float32))
    return density.astype(jnp.bfloat16)
```

```python
import functools

import jax
import jax.numpy as jnp
from jax import lax
from jax.experimental import pallas as pl
from jax.experimental.pallas import tpu as pltpu
from jax.sharding import PartitionSpec as P

CHUNKS = 2
PARTS = 4

NEAR_BY_X = 2
FAR_BY_X = 3
ORDER = (0, 3, 1, 2)
OWN, ACROSS, BESIDE, BEYOND, FOURTH, TRANSIT = range(6)


def relay_kernel(
    panels, lags,
    counts_ref, pairs_hbm, send_hbm, local_ref, weights_ref, incident_ref, near_ref,
    out_ref,
    pairs_ref, send_ref, scalar_sem,
    windows, weights, near, incident, right, running, partial_value, landed,
    send_sem, recv_sem, local_sem, weight_sem, near_sem, incident_sem,
    sum_send_sem, sum_recv_sem, chain_sem,
):
    here = lax.axis_index("panel")
    lag = lax.axis_index("lag")
    offsets = send_ref.shape[1]
    reach = offsets // 2
    blocks, piece, fields = windows[0].shape[1:]
    depth = piece * PARTS
    count = weights.shape[0]
    own = incident.shape[0]
    places = panels // 4
    x = lax.rem(here, 2)
    y = lax.rem(here // 2, 2)
    way = 1 - 2 * y
    z = here // 4
    at_chain = jnp.where(y == 0, z, places - 1 - z)
    feeds_near = x == y

    def panel(steps):
        return lax.rem(here + steps + panels, panels)

    to_x = panel(1 - 2 * x)
    to_y = panel(2 * way)
    to_z = panel(4 * way)
    from_z = panel(-4 * way)

    def rows_of(part):
        return pl.ds(part * piece, piece)

    locals_here = [
        pltpu.make_async_copy(
            local_ref.at[0, :, rows_of(part)], windows[part].at[OWN], local_sem.at[part]
        )
        for part in range(PARTS)
    ]
    for copy in locals_here:
        copy.start()
    scalar_copies = [
        pltpu.make_async_copy(source, target, scalar_sem.at[i])
        for i, (source, target) in enumerate(
            [(pairs_hbm, pairs_ref), (send_hbm, send_ref)]
        )
    ]
    for copy in scalar_copies:
        copy.start()
    weight_copies = [
        pltpu.make_async_copy(weights_ref.at[0, 0, k], weights.at[k], weight_sem.at[k])
        for k in range(count)
    ]

    barrier = pltpu.get_barrier_semaphore()

    def greet(semaphore, **device):
        pl.semaphore_signal(
            semaphore, inc=1, device_id=device, device_id_type=pl.DeviceIdType.MESH
        )

    greet(barrier, panel=to_x)
    greet(barrier, panel=to_y)

    @pl.when(at_chain > 0)
    def _():
        greet(barrier, panel=from_z)

    for ahead in range(1, lags):
        greet(barrier, lag=lax.rem(lag + ahead, lags))
    pl.semaphore_wait(
        barrier, 2 + lags - 1 + jnp.where(at_chain < places - 1, 1, 0).astype(jnp.int32)
    )
    for copy in locals_here:
        copy.wait()

    def copy_of(source, target, link, part, block, device):
        return pltpu.make_async_remote_copy(
            src_ref=windows[part].at[source, block],
            dst_ref=windows[part].at[target, block],
            send_sem=send_sem.at[link, part, block],
            recv_sem=recv_sem.at[target - 1, part, block],
            device_id={"panel": device},
            device_id_type=pl.DeviceIdType.MESH,
        )

    def by_x(part, block):
        return copy_of(OWN, ACROSS, 0, part, block, to_x)

    def by_y(part, block):
        return copy_of(OWN, BESIDE, 1, part, block, to_y)

    def by_z(part, block):
        return copy_of(BESIDE, BEYOND, 2, part, block, to_z)

    def fourth_by_x(part, block):
        return copy_of(jnp.where(feeds_near, BESIDE, BEYOND), FOURTH, 3, part, block, to_x)

    def fourth_by_y(part, block):
        return copy_of(
            ACROSS, jnp.where(feeds_near, FOURTH, TRANSIT), 4, part, block, to_y
        )

    def fourth_by_z(part, block):
        return copy_of(TRANSIT, FOURTH, 5, part, block, to_z)

    def landing(slot, part, block):
        return copy_of(slot, slot, 0, part, block, to_x)

    pieces = [(part, block) for part in range(PARTS) for block in range(blocks)]
    backward = pieces[::-1]
    for one, other in zip(backward, pieces):
        by_x(*one).start()
        by_y(*other).start()

    @pl.when(at_chain > 0)
    def _():
        pl.semaphore_wait(chain_sem, 1)

    @pl.when(at_chain < places - 1)
    def _():
        greet(chain_sem, panel=to_z)

    near_copy = pltpu.make_async_copy(near_ref, near, near_sem)
    incident_copy = pltpu.make_async_copy(incident_ref, incident, incident_sem)
    for copy in weight_copies:
        copy.start()
    incident_copy.start()
    near_copy.start()

    behind = 3
    total_steps = len(pieces) + behind
    for step in range(total_steps):
        if step < len(pieces):
            part, block = backward[step]
            landing(ACROSS, part, block).wait_recv()
            if part >= max(NEAR_BY_X, FAR_BY_X):
                fourth_by_y(part, block).start()
            elif part >= NEAR_BY_X:
                @pl.when(feeds_near)
                def _():
                    fourth_by_y(part, block).start()
            elif part >= FAR_BY_X:
                @pl.when(jnp.logical_not(feeds_near))
                def _():
                    fourth_by_y(part, block).start()
            part, block = pieces[step]
            landing(BESIDE, part, block).wait_recv()
            by_z(part, block).start()
            if part < NEAR_BY_X:
                @pl.when(feeds_near)
                def _():
                    fourth_by_x(part, block).start()
        if step >= behind:
            part, block = pieces[step - behind]

            @pl.when(jnp.logical_not(feeds_near))
            def _():
                landing(BEYOND, part, block).wait_recv()
                if part < FAR_BY_X:
                    fourth_by_x(part, block).start()

    @pl.when(feeds_near)
    def _():
        for part, block in backward:
            if part >= FAR_BY_X:
                landing(TRANSIT, part, block).wait_recv()
                fourth_by_z(part, block).start()
        for part, block in pieces:
            landing(BEYOND, part, block).wait_recv()

    for copy in scalar_copies + weight_copies:
        copy.wait()
    incident_copy.wait()
    near_copy.wait()

    live = counts_ref[0, 0]
    readers = right.shape[2] // fields
    chosen = []
    for k in range(count):
        offset = pairs_ref[0, 0, 0, k]
        slot = pairs_ref[0, 1, 0, k]
        reader = pairs_ref[0, 2, 0, k]
        steps = offset - reach
        block = send_ref[0, offset, slot, panel(steps)]
        place = jnp.where(
            steps == 0, OWN,
            jnp.where(
                steps == 1 - 2 * x, ACROSS,
                jnp.where(
                    steps == 2 * way, BESIDE, jnp.where(steps == -2 * way, BEYOND, FOURTH)
                ),
            ),
        )
        chosen.append((place, block, reader))

    def arrive(part):
        for block in range(blocks):
            landing(FOURTH, part, block).wait_recv()
        for k, (place, block, reader) in enumerate(chosen):
            value = windows[part][place, block]
            for r in range(readers):
                kept = jnp.logical_and(reader == r, k < live)
                right[part, k * piece:(k + 1) * piece, r * fields:(r + 1) * fields] = jnp.where(
                    kept, value, jnp.zeros_like(value)
                )

    def product(part, at):
        left = jnp.concatenate(
            [weights[k, at, part * piece:(part + 1) * piece] for k in range(count)], axis=1
        )
        return jnp.dot(left, right[part], preferred_element_type=jnp.float32)

    rows = depth // CHUNKS
    sums = []
    for part in ORDER[:-1]:
        arrive(part)
        for chunk in range(CHUNKS):
            at = slice(chunk * rows, (chunk + 1) * rows)
            term = product(part, at)
            running[at, :] = term if part == ORDER[0] else running[at, :] + term
    arrive(ORDER[-1])
    for chunk in range(CHUNKS):
        at = slice(chunk * rows, (chunk + 1) * rows)
        total = running[at, :] + product(ORDER[-1], at)
        for r in range(readers):
            partial_value[r, at, :] = total[:, r * fields:(r + 1) * fields]
        for ahead in range(1, lags):
            other = lax.rem(lag + ahead, lags)
            copy = pltpu.make_async_remote_copy(
                src_ref=partial_value.at[pl.ds(other * own, own), pl.ds(chunk * rows, rows)],
                dst_ref=landed.at[ahead - 1, :, pl.ds(chunk * rows, rows)],
                send_sem=sum_send_sem.at[ahead - 1, chunk],
                recv_sem=sum_recv_sem.at[ahead - 1, chunk],
                device_id={"lag": other},
                device_id_type=pl.DeviceIdType.MESH,
            )
            copy.start()
            sums.append(copy)
    for part, block in pieces:
        by_x(part, block).wait_send()
        by_y(part, block).wait_send()
        by_z(part, block).wait_send()

    @pl.when(feeds_near)
    def _():
        for part, block in pieces:
            if part < NEAR_BY_X:
                fourth_by_x(part, block).wait_send()
            else:
                fourth_by_y(part, block).wait_send()
            if part >= FAR_BY_X:
                fourth_by_z(part, block).wait_send()

    @pl.when(jnp.logical_not(feeds_near))
    def _():
        for part, block in pieces:
            if part < FAR_BY_X:
                fourth_by_x(part, block).wait_send()
            else:
                fourth_by_y(part, block).wait_send()

    for copy in sums:
        copy.wait_recv()
    for j in range(own):
        summed = partial_value[lag * own + j]
        for ahead in range(1, lags):
            summed = summed + landed[ahead - 1, j]
        remainder = (incident[j].astype(jnp.float32) - summed).astype(jnp.bfloat16)
        out_ref[j] = jnp.dot(
            near[j], remainder, preferred_element_type=jnp.float32
        ).astype(out_ref.dtype)
    for copy in sums:
        copy.wait_send()


def relayed(panels, lags, history, weights, pairs, counts, send_list, incident, near_inverse):
    readers, depth, fields = history.shape[1:]
    count = weights.shape[2]
    own = incident.shape[0]
    piece = depth // PARTS
    in_hbm = pl.BlockSpec(memory_space=pltpu.HBM)
    dma = pltpu.SemaphoreType.DMA
    held = [
        pltpu.with_memory_space_constraint(operand, pltpu.HBM)
        for operand in (
            jnp.transpose(pairs, (0, 3, 1, 2)), jnp.transpose(send_list, (1, 2, 3, 0)),
            history, weights, incident, near_inverse,
        )
    ]
    return pl.pallas_call(
        functools.partial(relay_kernel, panels, lags),
        out_shape=pltpu.VMEM(incident.shape, jnp.bfloat16),
        in_specs=[pl.BlockSpec(memory_space=pltpu.SMEM)] + [in_hbm] * 6,
        out_specs=pl.BlockSpec(memory_space=pltpu.VMEM),
        scratch_shapes=[
            *[pltpu.SMEM(operand.shape, operand.dtype) for operand in held[:2]],
            dma((2,)),
            [pltpu.VMEM((TRANSIT + 1, readers, piece, fields), history.dtype)] * PARTS,
            pltpu.VMEM(weights.shape[2:], weights.dtype),
            pltpu.VMEM(near_inverse.shape, near_inverse.dtype),
            pltpu.VMEM(incident.shape, incident.dtype),
            pltpu.VMEM((PARTS, count * piece, readers * fields), history.dtype),
            pltpu.VMEM((depth, readers * fields), jnp.float32),
            pltpu.VMEM((readers, depth, fields), jnp.float32),
            pltpu.VMEM((lags - 1, own, depth, fields), jnp.float32),
            dma((6, PARTS, readers)),
            dma((TRANSIT, PARTS, readers)),
            dma((PARTS,)),
            dma((count,)),
            dma,
            dma,
            dma((lags - 1, CHUNKS)),
            dma((lags - 1, CHUNKS)),
            pltpu.SemaphoreType.REGULAR,
        ],
        compiler_params=pltpu.CompilerParams(
            collective_id=0, has_side_effects=True, vmem_limit_bytes=48 * 1024 * 1024
        ),
    )(counts, *held)


def step_kernel(
    relay, panels, lags,
    pairs_ref, counts_ref, send_ref, local_ref, weights_ref, incident_ref, near_ref,
    out_ref,
    windows, weights, near, incident, right, running, partial_value, landed,
    send_sem, recv_sem, local_sem, weight_sem, near_sem, incident_sem,
    sum_send_sem, sum_recv_sem,
):
    here = lax.axis_index("panel")
    lag = lax.axis_index("lag")
    offsets = send_ref.shape[1]
    reach = offsets // 2
    blocks, piece, fields = windows[0].shape[1:]
    depth = piece * PARTS
    count = weights.shape[0]
    own = incident.shape[0]
    side = 2 * lax.rem(here, 2) - 1

    def panel(steps):
        return lax.rem(here + steps + panels, panels)

    def rows_of(part):
        return pl.ds(part * piece, piece)

    def outgoing(steps, part):
        if relay:
            return windows[part].at[0]
        return local_ref.at[reach - steps, :, rows_of(part)]

    source_here = local_ref.at[0] if relay else local_ref.at[reach]
    locals_here = [
        pltpu.make_async_copy(
            source_here.at[:, rows_of(part)], windows[part].at[0], local_sem.at[part]
        )
        for part in range(PARTS)
    ]
    for copy in locals_here:
        copy.start()
    weight_copies = [
        pltpu.make_async_copy(weights_ref.at[0, 0, k], weights.at[k], weight_sem.at[k])
        for k in range(count)
    ]

    barrier = pltpu.get_barrier_semaphore()
    greeted = [-side, 2 * side, -2 * side] + ([] if relay else [side])
    for steps in greeted:
        pl.semaphore_signal(
            barrier, inc=1, device_id={"panel": panel(steps)},
            device_id_type=pl.DeviceIdType.MESH,
        )
    for ahead in range(1, lags):
        pl.semaphore_signal(
            barrier, inc=1, device_id={"lag": lax.rem(lag + ahead, lags)},
            device_id_type=pl.DeviceIdType.MESH,
        )
    pl.semaphore_wait(barrier, len(greeted) + lags - 1)
    for copy in locals_here:
        copy.wait()

    def send(source, slot, part, steps):
        copy = pltpu.make_async_remote_copy(
            src_ref=source,
            dst_ref=windows[part].at[slot],
            send_sem=send_sem.at[slot - 1, part],
            recv_sem=recv_sem.at[slot - 1, part],
            device_id={"panel": panel(steps)},
            device_id_type=pl.DeviceIdType.MESH,
        )
        copy.start()
        return copy

    first, second, partner, passed = [], [], [], []
    lead = PARTS // 2
    for step in range(PARTS + lead):
        if step < PARTS:
            first.append(send(outgoing(2 * side, step), 3, step, 2 * side))
            partner.append(send(outgoing(-side, step), 4, step, -side))
        if step >= lead:
            part = step - lead
            second.append(send(outgoing(-2 * side, part), 2, part, -2 * side))
    near_copy = pltpu.make_async_copy(near_ref, near, near_sem)
    incident_copy = pltpu.make_async_copy(incident_ref, incident, incident_sem)
    for copy in weight_copies:
        copy.start()
    incident_copy.start()
    near_copy.start()
    def pass_on(part):
        if relay:
            first[part].wait_recv()
            passed.append(send(windows[part].at[3], 1, part, -side))
        else:
            passed.append(send(outgoing(side, part), 1, part, side))

    for part in range(PARTS):
        pass_on(part)
    for copy in weight_copies:
        copy.wait()
    incident_copy.wait()
    near_copy.wait()

    live = counts_ref[0, 0]
    readers = right.shape[2] // fields
    chosen = []
    for k in range(count):
        offset = pairs_ref[0, 0, 0, k]
        slot = pairs_ref[0, 1, 0, k]
        reader = pairs_ref[0, 2, 0, k]
        if relay:
            block = send_ref[0, offset, slot, panel(offset - reach)]
        else:
            block = slot
        place = lax.rem((offset - reach) * side + offsets, offsets)
        chosen.append((place, block, reader))

    def arrive(part):
        if not relay:
            first[part].wait_recv()
        partner[part].wait_recv()
        second[part].wait_recv()
        passed[part].wait_recv()
        for k, (place, block, reader) in enumerate(chosen):
            value = windows[part][place, block]
            for r in range(readers):
                kept = jnp.logical_and(reader == r, k < live)
                right[part, k * piece:(k + 1) * piece, r * fields:(r + 1) * fields] = jnp.where(
                    kept, value, jnp.zeros_like(value)
                )

    def product(part, at):
        left = jnp.concatenate(
            [weights[k, at, part * piece:(part + 1) * piece] for k in range(count)], axis=1
        )
        return jnp.dot(left, right[part], preferred_element_type=jnp.float32)

    rows = depth // CHUNKS
    sums = []
    for part in range(PARTS - 1):
        arrive(part)
        for chunk in range(CHUNKS):
            at = slice(chunk * rows, (chunk + 1) * rows)
            term = product(part, at)
            running[at, :] = term if part == 0 else running[at, :] + term
    arrive(PARTS - 1)
    for chunk in range(CHUNKS):
        at = slice(chunk * rows, (chunk + 1) * rows)
        total = running[at, :] + product(PARTS - 1, at)
        for r in range(readers):
            partial_value[r, at, :] = total[:, r * fields:(r + 1) * fields]
        for ahead in range(1, lags):
            other = lax.rem(lag + ahead, lags)
            copy = pltpu.make_async_remote_copy(
                src_ref=partial_value.at[pl.ds(other * own, own), pl.ds(chunk * rows, rows)],
                dst_ref=landed.at[ahead - 1, :, pl.ds(chunk * rows, rows)],
                send_sem=sum_send_sem.at[ahead - 1, chunk],
                recv_sem=sum_recv_sem.at[ahead - 1, chunk],
                device_id={"lag": other},
                device_id_type=pl.DeviceIdType.MESH,
            )
            copy.start()
            sums.append(copy)
    for copy in first + partner + second + passed:
        copy.wait_send()
    for copy in sums:
        copy.wait_recv()
    for j in range(own):
        summed = partial_value[lag * own + j]
        for ahead in range(1, lags):
            summed = summed + landed[ahead - 1, j]
        remainder = (incident[j].astype(jnp.float32) - summed).astype(jnp.bfloat16)
        out_ref[j] = jnp.dot(
            near[j], remainder, preferred_element_type=jnp.float32
        ).astype(out_ref.dtype)
    for copy in sums:
        copy.wait_send()


def on_device(panels, lags, history, weights, pairs, counts, send_list, incident, near_inverse):
    readers, depth, fields = history.shape[1:]
    offsets, slots = send_list.shape[2:]
    assert offsets == 5 and panels % 2 == 0 and panels > offsets
    count = weights.shape[2]
    own = incident.shape[0]
    if readers <= slots and panels % 4 == 0 and panels > 8:
        return relayed(
            panels, lags, history, weights, pairs, counts, send_list, incident, near_inverse
        )
    relay = readers <= slots
    blocks = readers if relay else slots
    local = history
    if not relay:
        here = lax.axis_index("panel")
        mine = lax.dynamic_index_in_dim(send_list, here, 0, keepdims=False)[0]
        local = jnp.take(history[0], mine.reshape(-1), axis=0).reshape(
            (offsets, slots, depth, fields)
        )
    anywhere = pl.BlockSpec(memory_space=pl.ANY)
    scalars = pl.BlockSpec(memory_space=pltpu.SMEM)
    dma = pltpu.SemaphoreType.DMA
    return pl.pallas_call(
        functools.partial(step_kernel, relay, panels, lags),
        out_shape=jax.ShapeDtypeStruct(incident.shape, jnp.bfloat16),
        in_specs=[scalars] * 3 + [anywhere] * 4,
        out_specs=pl.BlockSpec(memory_space=pltpu.VMEM),
        scratch_shapes=[
            [pltpu.VMEM((offsets, blocks, depth // PARTS, fields), history.dtype)] * PARTS,
            pltpu.VMEM(weights.shape[2:], weights.dtype),
            pltpu.VMEM(near_inverse.shape, near_inverse.dtype),
            pltpu.VMEM(incident.shape, incident.dtype),
            pltpu.VMEM((PARTS, count * depth // PARTS, readers * fields), history.dtype),
            pltpu.VMEM((depth, readers * fields), jnp.float32),
            pltpu.VMEM((readers, depth, fields), jnp.float32),
            pltpu.VMEM((lags - 1, own, depth, fields), jnp.float32),
            dma((offsets - 1, PARTS)),
            dma((offsets - 1, PARTS)),
            dma((PARTS,)),
            dma((count,)),
            dma,
            dma,
            dma((lags - 1, CHUNKS)),
            dma((lags - 1, CHUNKS)),
        ],
        compiler_params=pltpu.CompilerParams(
            collective_id=0, has_side_effects=True, vmem_limit_bytes=67043328
        ),
    )(jnp.transpose(pairs, (0, 3, 1, 2)), counts, jnp.transpose(send_list, (1, 2, 3, 0)), local, weights, incident, near_inverse)


def solution(mesh):
    return jax.shard_map(
        functools.partial(on_device, mesh.shape["panel"], mesh.shape["lag"]),
        mesh=mesh,
        in_specs=(
            P("lag", "panel", None, None),
            P("panel", "lag", None, None, None),
            P("panel", "lag", None, None),
            P("panel", "lag"),
            P(None, "lag", None, None),
            P(("panel", "lag"), None, None),
            P(("panel", "lag"), None, None),
        ),
        out_specs=P(("panel", "lag"), None, None),
        check_vma=False,
    )
```

```python
import functools

import jax
import jax.numpy as jnp
from jax import lax
from jax.experimental import pallas as pl
from jax.experimental.pallas import tpu as pltpu
from jax.sharding import PartitionSpec as P

CHUNKS = 2
PARTS = 4

NEAR_BY_X = 2
FAR_BY_X = 3
RING_OWN = 1
DIRECT = 2
OWN, ACROSS, BESIDE, BEYOND, FOURTH, TRANSIT = range(6)
BEHIND = 5
ASIDE = 3
LATE_GREETING = 3


def relay_kernel(
    panels, lags,
    counts_ref, pairs_hbm, send_hbm, local_ref, weights_ref, incident_ref, near_ref,
    out_ref,
    pairs_ref, send_ref, scalar_sem,
    windows, weights, near, incident, running, partial_value, landed,
    send_sem, recv_sem, local_sem, weight_sem, near_sem, incident_sem,
    sum_send_sem, sum_recv_sem, chain_sem,
):
    here = lax.axis_index("panel")
    lag = lax.axis_index("lag")
    offsets, slots = send_ref.shape[1:3]
    reach = offsets // 2
    blocks, piece, fields = windows[0].shape[1:]
    depth = piece * PARTS
    count = weights.shape[0]
    own = incident.shape[0]
    places = panels // 4
    x = lax.rem(here, 2)
    y = lax.rem(here // 2, 2)
    way = 1 - 2 * y
    z = here // 4
    at_chain = jnp.where(y == 0, z, places - 1 - z)
    first = at_chain == 0
    last = at_chain == places - 1
    feeds_near = x == y
    feeds_far = x != y
    start = jnp.logical_and(y == 0, first)
    before_end = jnp.logical_and(y == 0, last)
    end = jnp.logical_and(y == 1, first)
    waits_long = jnp.logical_and(y == 1, last)
    near_end = jnp.logical_and(feeds_near, last)
    skips_z = jnp.logical_and(before_end, feeds_far)

    def panel(steps):
        return lax.rem(here + steps + panels, panels)

    to_x = panel(1 - 2 * x)
    to_y = panel(2 * way)
    to_z = panel(4 * way)
    from_z = panel(-4 * way)
    to_start = panel(2)
    to_opening = panel(3)

    def rows_of(part):
        return pl.ds(part * piece, piece)

    locals_here = [
        pltpu.make_async_copy(
            local_ref.at[0, :, rows_of(part)], windows[part].at[OWN], local_sem.at[part]
        )
        for part in range(PARTS)
    ]
    for copy in locals_here:
        copy.start()
    scalar_copies = [
        pltpu.make_async_copy(source, target, scalar_sem.at[i])
        for i, (source, target) in enumerate([(pairs_hbm, pairs_ref), (send_hbm, send_ref)])
    ]
    for copy in scalar_copies:
        copy.start()
    weight_copies = [
        pltpu.make_async_copy(weights_ref.at[0, 0, k], weights.at[k], weight_sem.at[k])
        for k in range(count)
    ]
    near_copy = pltpu.make_async_copy(near_ref, near, near_sem)
    incident_copy = pltpu.make_async_copy(incident_ref, incident, incident_sem)

    barrier = pltpu.get_barrier_semaphore()

    def greet(semaphore, **device):
        pl.semaphore_signal(
            semaphore, inc=1, device_id=device, device_id_type=pl.DeviceIdType.MESH
        )

    greet(barrier, panel=to_x)
    greet(barrier, panel=to_y)

    @pl.when(jnp.logical_not(end))
    def _():
        greet(barrier, panel=from_z)

    @pl.when(start)
    def _():
        greet(barrier, panel=panel(-2))

        @pl.when(feeds_near)
        def _():
            greet(barrier, panel=panel(-3))

    for ahead in range(1, lags):
        greet(barrier, lag=lax.rem(lag + ahead, lags))
    pl.semaphore_wait(
        barrier,
        2 + lags - 1 + jnp.where(waits_long, 0, jnp.where(jnp.logical_or(end, skips_z), 2, 1)).astype(jnp.int32),
    )
    for copy in locals_here:
        copy.wait()

    def copy_of(source, target, link, part, block, device):
        return pltpu.make_async_remote_copy(
            src_ref=windows[part].at[source, block],
            dst_ref=windows[part].at[target, block],
            send_sem=send_sem.at[link, part, block],
            recv_sem=recv_sem.at[target - 1, part, block],
            device_id={"panel": device},
            device_id_type=pl.DeviceIdType.MESH,
        )

    def by_x(part, block):
        return copy_of(OWN, ACROSS, 0, part, block, to_x)

    def by_y(part, block):
        return copy_of(OWN, BESIDE, 1, part, block, to_y)

    def by_z(part, block):
        return copy_of(BESIDE, BEYOND, 2, part, block, to_z)

    def fourth_by_x(part, block):
        return copy_of(jnp.where(feeds_near, BESIDE, BEYOND), FOURTH, 3, part, block, to_x)

    def fourth_by_y(part, block):
        return copy_of(
            ACROSS, jnp.where(feeds_near, FOURTH, TRANSIT), 4, part, block, to_y
        )

    def fourth_by_z(part, block):
        return copy_of(TRANSIT, FOURTH, 5, part, block, to_z)

    def by_ring(part, block):
        return copy_of(OWN, BEYOND, 6, part, block, to_start)

    def fourth_by_ring(part, block):
        return copy_of(ACROSS, FOURTH, 7, part, block, to_start)

    def fourth_at_once(part, block):
        return copy_of(BESIDE, FOURTH, 8, part, block, to_opening)

    def landing(slot, part, block):
        return copy_of(slot, slot, 0, part, block, to_x)

    pieces = [(part, block) for part in range(PARTS) for block in range(blocks)]
    backward = pieces[::-1]

    for one, other in zip(backward, pieces):
        by_y(*other).start()
        by_x(*one).start()
        if other[0] < RING_OWN:
            @pl.when(jnp.logical_and(end, feeds_near))
            def _():
                by_ring(*other).start()

    for copy in weight_copies:
        copy.start()
    incident_copy.start()
    near_copy.start()

    def pass_greeting():
        @pl.when(jnp.logical_not(first))
        def _():
            pl.semaphore_wait(chain_sem, 1)

        @pl.when(jnp.logical_not(last))
        def _():
            greet(chain_sem, panel=to_z)

    @pl.when(jnp.logical_and(y == 1, at_chain <= 1))
    def _():
        pass_greeting()

    for copy in scalar_copies:
        copy.wait()
    live = counts_ref[0, 0]
    readers = partial_value.shape[0]
    steps_of = (0, 1 - 2 * x, 2 * way, -2 * way, 2 * x - 1)
    chosen = []
    for steps in steps_of:
        row = []
        for slot in range(slots):
            index, found, reader = 0, 0, 0
            for k in range(count):
                hit = jnp.logical_and(
                    jnp.logical_and(
                        pairs_ref[0, 0, 0, k] == reach + steps, pairs_ref[0, 1, 0, k] == slot
                    ),
                    k < live,
                )
                index = jnp.where(hit, k, index)
                found = jnp.where(hit, 1, found)
                reader = jnp.where(hit, pairs_ref[0, 2, 0, k], reader)
            block = send_ref[0, reach + steps, slot, panel(steps)]
            row.append((index, found, reader, block))
        chosen.append(row)
    for copy in weight_copies:
        copy.wait()

    def product(terms, at):
        left, right = [], []
        for place, part in terms:
            for index, found, reader, block in chosen[place]:
                left.append(weights[index, at, part * piece:(part + 1) * piece])
                value = windows[part][place, 0]
                for b in range(1, blocks):
                    value = jnp.where(block == b, windows[part][place, b], value)
                right.append(
                    jnp.concatenate(
                        [
                            jnp.where(
                                jnp.logical_and(found == 1, reader == r),
                                value, jnp.zeros_like(value),
                            )
                            for r in range(readers)
                        ],
                        axis=1,
                    )
                )
        return jnp.dot(
            jnp.concatenate(left, axis=1), jnp.concatenate(right, axis=0),
            preferred_element_type=jnp.float32,
        )

    rows = depth // CHUNKS
    chunks = [slice(chunk * rows, (chunk + 1) * rows) for chunk in range(CHUNKS)]

    def add(*terms, fresh=False):
        for at in chunks:
            term = product(terms, at)
            running[at, :] = term if fresh else running[at, :] + term

    add(*[(OWN, part) for part in range(PARTS)], fresh=True)

    for step in range(len(pieces) + max(ASIDE, BEHIND)):
        if step < len(pieces):
            part, block = pieces[step]

            @pl.when(end)
            def _():
                landing(ACROSS, *backward[step]).wait_recv()
                if backward[step][0] >= DIRECT:
                    @pl.when(feeds_far)
                    def _():
                        fourth_by_ring(*backward[step]).start()

            landing(BESIDE, part, block).wait_recv()
            if part < DIRECT:
                @pl.when(skips_z)
                def _():
                    fourth_at_once(part, block).start()

            if step < LATE_GREETING:
                @pl.when(
                    jnp.logical_not(
                        jnp.logical_or(waits_long, skips_z) if part < RING_OWN else waits_long
                    )
                )
                def _():
                    by_z(part, block).start()
            else:
                if step == LATE_GREETING:
                    @pl.when(waits_long)
                    def _():
                        pass_greeting()
                        for missed in pieces[:step]:
                            by_z(*missed).start()

                @pl.when(jnp.logical_not(skips_z) if part < RING_OWN else here >= 0)
                def _():
                    by_z(part, block).start()

            @pl.when(feeds_near if part < NEAR_BY_X else near_end)
            def _():
                fourth_by_x(part, block).start()

        if ASIDE <= step < len(pieces) + ASIDE:
            turn = step - ASIDE
            part, block = backward[turn]

            @pl.when(jnp.logical_not(end))
            def _():
                landing(ACROSS, part, block).wait_recv()
                if part >= NEAR_BY_X:
                    @pl.when(jnp.logical_and(feeds_near, jnp.logical_not(first)))
                    def _():
                        fourth_by_y(part, block).start()

                if part >= FAR_BY_X:
                    @pl.when(feeds_far)
                    def _():
                        fourth_by_y(part, block).start()

            if turn % blocks == blocks - 1:
                add((BESIDE, turn // blocks))
        if step == 1:
            @pl.when(jnp.logical_and(y == 1, jnp.logical_and(at_chain > 1, jnp.logical_not(last))))
            def _():
                pass_greeting()
        if BEHIND <= step < len(pieces) + BEHIND:
            part, block = pieces[step - BEHIND]

            @pl.when(jnp.logical_and(feeds_far, jnp.logical_not(first)))
            def _():
                landing(BEYOND, part, block).wait_recv()
                if part < FAR_BY_X:
                    fourth_by_x(part, block).start()

    @pl.when(jnp.logical_and(feeds_near, jnp.logical_not(before_end)))
    def _():
        for part, block in backward:
            if part >= FAR_BY_X:
                landing(TRANSIT, part, block).wait_recv()
                fourth_by_z(part, block).start()

    def arrive(place, part):
        if place == BEYOND:
            @pl.when(jnp.logical_or(feeds_near, first))
            def _():
                for block in range(blocks):
                    landing(place, part, block).wait_recv()

            if part < FAR_BY_X:
                @pl.when(jnp.logical_and(end, feeds_far))
                def _():
                    for block in range(blocks):
                        fourth_by_x(part, block).start()
        else:
            for block in range(blocks):
                landing(place, part, block).wait_recv()

    add(*[(ACROSS, part) for part in range(PARTS)])
    order = [(BEYOND, 0)]
    for part in range(1, PARTS):
        order += [(BEYOND, part), (FOURTH, part - 1)]
    order.append((FOURTH, PARTS - 1))
    for place, part in order[:-1]:
        arrive(place, part)
        add((place, part))
    incident_copy.wait()
    near_copy.wait()
    arrive(*order[-1])
    sums = []
    for chunk, at in enumerate(chunks):
        total = running[at, :] + product(order[-1:], at)
        for r in range(readers):
            partial_value[r, at, :] = total[:, r * fields:(r + 1) * fields]
        for ahead in range(1, lags):
            other = lax.rem(lag + ahead, lags)
            copy = pltpu.make_async_remote_copy(
                src_ref=partial_value.at[pl.ds(other * own, own), pl.ds(chunk * rows, rows)],
                dst_ref=landed.at[ahead - 1, :, pl.ds(chunk * rows, rows)],
                send_sem=sum_send_sem.at[ahead - 1, chunk],
                recv_sem=sum_recv_sem.at[ahead - 1, chunk],
                device_id={"lag": other},
                device_id_type=pl.DeviceIdType.MESH,
            )
            copy.start()
            sums.append(copy)
    far_inner = jnp.logical_and(feeds_far, jnp.logical_not(first))
    for part, block in pieces:
        by_x(part, block).wait_send()
        by_y(part, block).wait_send()

        @pl.when(jnp.logical_not(skips_z) if part < RING_OWN else here >= 0)
        def _():
            by_z(part, block).wait_send()

        near_x = feeds_near if part < NEAR_BY_X else near_end
        end_far = jnp.logical_and(end, feeds_far)
        far_x = jnp.logical_and(jnp.logical_or(far_inner, end_far), part < FAR_BY_X)

        @pl.when(jnp.logical_or(near_x, far_x))
        def _():
            fourth_by_x(part, block).wait_send()

        if part >= NEAR_BY_X:
            @pl.when(jnp.logical_and(feeds_near, jnp.logical_not(first)))
            def _():
                fourth_by_y(part, block).wait_send()

        if part >= FAR_BY_X:
            @pl.when(jnp.logical_and(feeds_far, jnp.logical_not(end)))
            def _():
                fourth_by_y(part, block).wait_send()

            @pl.when(jnp.logical_and(feeds_near, jnp.logical_not(before_end)))
            def _():
                fourth_by_z(part, block).wait_send()

        if part < RING_OWN:
            @pl.when(jnp.logical_and(end, feeds_near))
            def _():
                by_ring(part, block).wait_send()

        if part < DIRECT:
            @pl.when(skips_z)
            def _():
                fourth_at_once(part, block).wait_send()
        else:
            @pl.when(end_far)
            def _():
                fourth_by_ring(part, block).wait_send()

    solved = [None] * own
    for chunk, at in enumerate(chunks):
        for copy in sums[chunk * (lags - 1):(chunk + 1) * (lags - 1)]:
            copy.wait_recv()
        for j in range(own):
            summed = partial_value[lag * own + j, at]
            for ahead in range(1, lags):
                summed = summed + landed[ahead - 1, j, at]
            remainder = (incident[j, at].astype(jnp.float32) - summed).astype(jnp.bfloat16)
            term = jnp.dot(near[j, :, at], remainder, preferred_element_type=jnp.float32)
            solved[j] = term if chunk == 0 else solved[j] + term
    for j in range(own):
        out_ref[j] = solved[j].astype(out_ref.dtype)
    for copy in sums:
        copy.wait_send()


def relayed(panels, lags, history, weights, pairs, counts, send_list, incident, near_inverse):
    readers, depth, fields = history.shape[1:]
    count = weights.shape[2]
    own = incident.shape[0]
    piece = depth // PARTS
    in_hbm = pl.BlockSpec(memory_space=pltpu.HBM)
    dma = pltpu.SemaphoreType.DMA
    held = [
        pltpu.with_memory_space_constraint(operand, pltpu.HBM)
        for operand in (
            jnp.transpose(pairs, (0, 3, 1, 2)), jnp.transpose(send_list, (1, 2, 3, 0)),
            history, weights, incident, near_inverse,
        )
    ]
    return pl.pallas_call(
        functools.partial(relay_kernel, panels, lags),
        out_shape=pltpu.VMEM(incident.shape, jnp.bfloat16),
        in_specs=[pl.BlockSpec(memory_space=pltpu.SMEM)] + [in_hbm] * 6,
        out_specs=pl.BlockSpec(memory_space=pltpu.VMEM),
        scratch_shapes=[
            *[pltpu.SMEM(operand.shape, operand.dtype) for operand in held[:2]],
            dma((2,)),
            [pltpu.VMEM((TRANSIT + 1, readers, piece, fields), history.dtype)] * PARTS,
            pltpu.VMEM(weights.shape[2:], weights.dtype),
            pltpu.VMEM(near_inverse.shape, near_inverse.dtype),
            pltpu.VMEM(incident.shape, incident.dtype),
            pltpu.VMEM((depth, readers * fields), jnp.float32),
            pltpu.VMEM((readers, depth, fields), jnp.float32),
            pltpu.VMEM((lags - 1, own, depth, fields), jnp.float32),
            dma((9, PARTS, readers)),
            dma((TRANSIT, PARTS, readers)),
            dma((PARTS,)),
            dma((count,)),
            dma,
            dma,
            dma((lags - 1, CHUNKS)),
            dma((lags - 1, CHUNKS)),
            pltpu.SemaphoreType.REGULAR,
        ],
        compiler_params=pltpu.CompilerParams(
            collective_id=0, has_side_effects=True, vmem_limit_bytes=48 * 1024 * 1024
        ),
    )(counts, *held)


def step_kernel(
    relay, panels, lags,
    pairs_ref, counts_ref, send_ref, local_ref, weights_ref, incident_ref, near_ref,
    out_ref,
    windows, weights, near, incident, right, running, partial_value, landed,
    send_sem, recv_sem, local_sem, weight_sem, near_sem, incident_sem,
    sum_send_sem, sum_recv_sem,
):
    here = lax.axis_index("panel")
    lag = lax.axis_index("lag")
    offsets = send_ref.shape[1]
    reach = offsets // 2
    blocks, piece, fields = windows[0].shape[1:]
    depth = piece * PARTS
    count = weights.shape[0]
    own = incident.shape[0]
    side = 2 * lax.rem(here, 2) - 1

    def panel(steps):
        return lax.rem(here + steps + panels, panels)

    def rows_of(part):
        return pl.ds(part * piece, piece)

    def outgoing(steps, part):
        if relay:
            return windows[part].at[0]
        return local_ref.at[reach - steps, :, rows_of(part)]

    source_here = local_ref.at[0] if relay else local_ref.at[reach]
    locals_here = [
        pltpu.make_async_copy(
            source_here.at[:, rows_of(part)], windows[part].at[0], local_sem.at[part]
        )
        for part in range(PARTS)
    ]
    for copy in locals_here:
        copy.start()
    weight_copies = [
        pltpu.make_async_copy(weights_ref.at[0, 0, k], weights.at[k], weight_sem.at[k])
        for k in range(count)
    ]

    barrier = pltpu.get_barrier_semaphore()
    greeted = [-side, 2 * side, -2 * side] + ([] if relay else [side])
    for steps in greeted:
        pl.semaphore_signal(
            barrier, inc=1, device_id={"panel": panel(steps)},
            device_id_type=pl.DeviceIdType.MESH,
        )
    for ahead in range(1, lags):
        pl.semaphore_signal(
            barrier, inc=1, device_id={"lag": lax.rem(lag + ahead, lags)},
            device_id_type=pl.DeviceIdType.MESH,
        )
    pl.semaphore_wait(barrier, len(greeted) + lags - 1)
    for copy in locals_here:
        copy.wait()

    def send(source, slot, part, steps):
        copy = pltpu.make_async_remote_copy(
            src_ref=source,
            dst_ref=windows[part].at[slot],
            send_sem=send_sem.at[slot - 1, part],
            recv_sem=recv_sem.at[slot - 1, part],
            device_id={"panel": panel(steps)},
            device_id_type=pl.DeviceIdType.MESH,
        )
        copy.start()
        return copy

    first, second, partner, passed = [], [], [], []
    lead = PARTS // 2
    for step in range(PARTS + lead):
        if step < PARTS:
            first.append(send(outgoing(2 * side, step), 3, step, 2 * side))
            partner.append(send(outgoing(-side, step), 4, step, -side))
        if step >= lead:
            part = step - lead
            second.append(send(outgoing(-2 * side, part), 2, part, -2 * side))
    near_copy = pltpu.make_async_copy(near_ref, near, near_sem)
    incident_copy = pltpu.make_async_copy(incident_ref, incident, incident_sem)
    for copy in weight_copies:
        copy.start()
    incident_copy.start()
    near_copy.start()
    def pass_on(part):
        if relay:
            first[part].wait_recv()
            passed.append(send(windows[part].at[3], 1, part, -side))
        else:
            passed.append(send(outgoing(side, part), 1, part, side))

    for part in range(PARTS):
        pass_on(part)
    for copy in weight_copies:
        copy.wait()
    incident_copy.wait()
    near_copy.wait()

    live = counts_ref[0, 0]
    readers = right.shape[2] // fields
    chosen = []
    for k in range(count):
        offset = pairs_ref[0, 0, 0, k]
        slot = pairs_ref[0, 1, 0, k]
        reader = pairs_ref[0, 2, 0, k]
        if relay:
            block = send_ref[0, offset, slot, panel(offset - reach)]
        else:
            block = slot
        place = lax.rem((offset - reach) * side + offsets, offsets)
        chosen.append((place, block, reader))

    def arrive(part):
        if not relay:
            first[part].wait_recv()
        partner[part].wait_recv()
        second[part].wait_recv()
        passed[part].wait_recv()
        for k, (place, block, reader) in enumerate(chosen):
            value = windows[part][place, block]
            for r in range(readers):
                kept = jnp.logical_and(reader == r, k < live)
                right[part, k * piece:(k + 1) * piece, r * fields:(r + 1) * fields] = jnp.where(
                    kept, value, jnp.zeros_like(value)
                )

    def product(part, at):
        left = jnp.concatenate(
            [weights[k, at, part * piece:(part + 1) * piece] for k in range(count)], axis=1
        )
        return jnp.dot(left, right[part], preferred_element_type=jnp.float32)

    rows = depth // CHUNKS
    sums = []
    for part in range(PARTS - 1):
        arrive(part)
        for chunk in range(CHUNKS):
            at = slice(chunk * rows, (chunk + 1) * rows)
            term = product(part, at)
            running[at, :] = term if part == 0 else running[at, :] + term
    arrive(PARTS - 1)
    for chunk in range(CHUNKS):
        at = slice(chunk * rows, (chunk + 1) * rows)
        total = running[at, :] + product(PARTS - 1, at)
        for r in range(readers):
            partial_value[r, at, :] = total[:, r * fields:(r + 1) * fields]
        for ahead in range(1, lags):
            other = lax.rem(lag + ahead, lags)
            copy = pltpu.make_async_remote_copy(
                src_ref=partial_value.at[pl.ds(other * own, own), pl.ds(chunk * rows, rows)],
                dst_ref=landed.at[ahead - 1, :, pl.ds(chunk * rows, rows)],
                send_sem=sum_send_sem.at[ahead - 1, chunk],
                recv_sem=sum_recv_sem.at[ahead - 1, chunk],
                device_id={"lag": other},
                device_id_type=pl.DeviceIdType.MESH,
            )
            copy.start()
            sums.append(copy)
    for copy in first + partner + second + passed:
        copy.wait_send()
    for copy in sums:
        copy.wait_recv()
    for j in range(own):
        summed = partial_value[lag * own + j]
        for ahead in range(1, lags):
            summed = summed + landed[ahead - 1, j]
        remainder = (incident[j].astype(jnp.float32) - summed).astype(jnp.bfloat16)
        out_ref[j] = jnp.dot(
            near[j], remainder, preferred_element_type=jnp.float32
        ).astype(out_ref.dtype)
    for copy in sums:
        copy.wait_send()


def on_device(panels, lags, history, weights, pairs, counts, send_list, incident, near_inverse):
    readers, depth, fields = history.shape[1:]
    offsets, slots = send_list.shape[2:]
    assert offsets == 5 and panels % 2 == 0 and panels > offsets
    count = weights.shape[2]
    own = incident.shape[0]
    if readers <= slots and panels % 4 == 0 and panels > 8:
        return relayed(
            panels, lags, history, weights, pairs, counts, send_list, incident, near_inverse
        )
    relay = readers <= slots
    blocks = readers if relay else slots
    local = history
    if not relay:
        here = lax.axis_index("panel")
        mine = lax.dynamic_index_in_dim(send_list, here, 0, keepdims=False)[0]
        local = jnp.take(history[0], mine.reshape(-1), axis=0).reshape(
            (offsets, slots, depth, fields)
        )
    anywhere = pl.BlockSpec(memory_space=pl.ANY)
    scalars = pl.BlockSpec(memory_space=pltpu.SMEM)
    dma = pltpu.SemaphoreType.DMA
    return pl.pallas_call(
        functools.partial(step_kernel, relay, panels, lags),
        out_shape=jax.ShapeDtypeStruct(incident.shape, jnp.bfloat16),
        in_specs=[scalars] * 3 + [anywhere] * 4,
        out_specs=pl.BlockSpec(memory_space=pltpu.VMEM),
        scratch_shapes=[
            [pltpu.VMEM((offsets, blocks, depth // PARTS, fields), history.dtype)] * PARTS,
            pltpu.VMEM(weights.shape[2:], weights.dtype),
            pltpu.VMEM(near_inverse.shape, near_inverse.dtype),
            pltpu.VMEM(incident.shape, incident.dtype),
            pltpu.VMEM((PARTS, count * depth // PARTS, readers * fields), history.dtype),
            pltpu.VMEM((depth, readers * fields), jnp.float32),
            pltpu.VMEM((readers, depth, fields), jnp.float32),
            pltpu.VMEM((lags - 1, own, depth, fields), jnp.float32),
            dma((offsets - 1, PARTS)),
            dma((offsets - 1, PARTS)),
            dma((PARTS,)),
            dma((count,)),
            dma,
            dma,
            dma((lags - 1, CHUNKS)),
            dma((lags - 1, CHUNKS)),
        ],
        compiler_params=pltpu.CompilerParams(
            collective_id=0, has_side_effects=True, vmem_limit_bytes=67043328
        ),
    )(jnp.transpose(pairs, (0, 3, 1, 2)), counts, jnp.transpose(send_list, (1, 2, 3, 0)), local, weights, incident, near_inverse)


def solution(mesh):
    return jax.shard_map(
        functools.partial(on_device, mesh.shape["panel"], mesh.shape["lag"]),
        mesh=mesh,
        in_specs=(
            P("lag", "panel", None, None),
            P("panel", "lag", None, None, None),
            P("panel", "lag", None, None),
            P("panel", "lag"),
            P(None, "lag", None, None),
            P(("panel", "lag"), None, None),
            P(("panel", "lag"), None, None),
        ),
        out_specs=P(("panel", "lag"), None, None),
        check_vma=False,
    )
```

```python
import functools

import jax
import jax.numpy as jnp
from jax import lax
from jax.experimental import pallas as pl
from jax.experimental.pallas import tpu as pltpu
from jax.sharding import PartitionSpec as P

CHUNKS = 2
PARTS = 4

NEAR_BY_X = 2
FAR_BY_X = 3
RING_OWN = 1
DIRECT = 2
STRAIGHT = (2,)
OWN, ACROSS, BESIDE, BEYOND, FOURTH, TRANSIT = range(6)
BEHIND = 5
ASIDE = 3
LATE_GREETING = 3


def relay_kernel(
    panels, lags,
    counts_ref, pairs_hbm, send_hbm, local_ref, weights_ref, incident_ref, near_ref,
    out_ref,
    pairs_ref, send_ref, scalar_sem,
    windows, weights, near, incident, running, partial_value, landed,
    send_sem, recv_sem, local_sem, weight_sem, near_sem, incident_sem,
    sum_send_sem, sum_recv_sem, chain_sem,
):
    here = lax.axis_index("panel")
    lag = lax.axis_index("lag")
    offsets, slots = send_ref.shape[1:3]
    reach = offsets // 2
    blocks, piece, fields = windows[0].shape[1:]
    depth = piece * PARTS
    count = weights.shape[0]
    own = incident.shape[0]
    places = panels // 4
    x = lax.rem(here, 2)
    y = lax.rem(here // 2, 2)
    way = 1 - 2 * y
    z = here // 4
    at_chain = jnp.where(y == 0, z, places - 1 - z)
    first = at_chain == 0
    last = at_chain == places - 1
    feeds_near = x == y
    feeds_far = x != y
    start = jnp.logical_and(y == 0, first)
    before_end = jnp.logical_and(y == 0, last)
    end = jnp.logical_and(y == 1, first)
    waits_long = jnp.logical_and(y == 1, last)
    near_end = jnp.logical_and(feeds_near, last)
    skips_z = jnp.logical_and(before_end, feeds_far)

    def panel(steps):
        return lax.rem(here + steps + panels, panels)

    to_x = panel(1 - 2 * x)
    to_y = panel(2 * way)
    to_z = panel(4 * way)
    from_z = panel(-4 * way)
    to_start = panel(2)
    to_first = panel(3)

    def rows_of(part):
        return pl.ds(part * piece, piece)

    locals_here = [
        pltpu.make_async_copy(
            local_ref.at[0, :, rows_of(part)], windows[part].at[OWN], local_sem
        )
        for part in range(PARTS)
    ]
    for copy in locals_here:
        copy.start()
    scalar_copies = [
        pltpu.make_async_copy(source, target, scalar_sem.at[i])
        for i, (source, target) in enumerate([(pairs_hbm, pairs_ref), (send_hbm, send_ref)])
    ]
    for copy in scalar_copies:
        copy.start()
    weight_copies = [
        pltpu.make_async_copy(weights_ref.at[0, 0], weights, weight_sem)
    ]
    near_copy = pltpu.make_async_copy(near_ref, near, near_sem)
    incident_copy = pltpu.make_async_copy(incident_ref, incident, incident_sem)

    barrier = pltpu.get_barrier_semaphore()

    def greet(semaphore, **device):
        pl.semaphore_signal(
            semaphore, inc=1, device_id=device, device_id_type=pl.DeviceIdType.MESH
        )

    greet(barrier, panel=to_x)
    greet(barrier, panel=to_y)

    @pl.when(jnp.logical_not(end))
    def _():
        greet(barrier, panel=from_z)

    @pl.when(start)
    def _():
        greet(barrier, panel=panel(-2))

        @pl.when(feeds_near)
        def _():
            greet(barrier, panel=panel(-3))
            greet(barrier, panel=panel(-1))

    for ahead in range(1, lags):
        greet(barrier, lag=lax.rem(lag + ahead, lags))
    pl.semaphore_wait(
        barrier,
        1
        + lags
        + jnp.where(
            waits_long, 0,
            jnp.where(end, jnp.where(feeds_near, 3, 2), jnp.where(skips_z, 2, 1)),
        ).astype(jnp.int32),
    )
    pltpu.make_async_copy(local_ref.at[0], local_ref.at[0], local_sem).wait()

    pieces = [(part, block) for part in range(PARTS) for block in range(blocks)]
    backward = pieces[::-1]

    alone = min(NEAR_BY_X, FAR_BY_X)
    each = PARTS * blocks
    relayed_across = (PARTS - alone) * blocks

    def arrival(target, part, block):
        if target == BESIDE:
            return part * blocks + block
        if target == BEYOND:
            return each + part * blocks + block
        if target == ACROSS:
            place = (part - alone) * blocks + block if part >= alone else relayed_across
            return 2 * each + place
        if target == FOURTH:
            return 2 * each + relayed_across + 1 + part
        return 2 * each + relayed_across + 1 + PARTS + (part - FAR_BY_X) * blocks + block

    def copy_of(source, target, link, part, block, device, lands=None):
        return pltpu.make_async_remote_copy(
            src_ref=windows[part].at[source, block],
            dst_ref=windows[part].at[target, block],
            send_sem=send_sem.at[link],
            recv_sem=recv_sem.at[arrival(target, part, block) if lands is None else lands],
            device_id={"panel": device},
            device_id_type=pl.DeviceIdType.MESH,
        )

    def by_x(part, block):
        return copy_of(OWN, ACROSS, 0, part, block, to_x)

    def by_y(part, block):
        return copy_of(OWN, BESIDE, 0, part, block, to_y)

    def by_z(part, block):
        return copy_of(BESIDE, BEYOND, 0, part, block, to_z)

    def fourth_by_x(part, block):
        return copy_of(jnp.where(feeds_near, BESIDE, BEYOND), FOURTH, 1, part, block, to_x)

    def fourth_by_y(part, block):
        if part < FAR_BY_X:
            return copy_of(ACROSS, FOURTH, 1, part, block, to_y)
        lands = jnp.where(
            feeds_near, arrival(FOURTH, part, block), arrival(TRANSIT, part, block)
        )
        return copy_of(
            ACROSS, jnp.where(feeds_near, FOURTH, TRANSIT), 1, part, block, to_y, lands
        )

    def fourth_by_z(part, block):
        return copy_of(TRANSIT, FOURTH, 1, part, block, to_z)

    def by_ring(part, block):
        return copy_of(OWN, BEYOND, 1, part, block, to_start)

    def fourth_by_ring(part, block):
        return copy_of(ACROSS, FOURTH, 1, part, block, to_start)

    def fourth_at_once(part, block):
        return copy_of(BESIDE, FOURTH, 1, part, block, to_first)

    def fourth_straight(part, block):
        return copy_of(OWN, FOURTH, 1, part, block, panel(1))

    def landing(slot, part, block):
        return copy_of(slot, slot, 0, part, block, to_x)

    def bulk(number, link, lands):
        rows = number * piece * fields // (2 * weights.shape[2])
        stretch = weights.at[pl.ds(0, 2), pl.ds(0, rows)]
        return pltpu.make_async_remote_copy(
            src_ref=stretch, dst_ref=stretch,
            send_sem=send_sem.at[link], recv_sem=recv_sem.at[lands],
            device_id={"panel": to_x}, device_id_type=pl.DeviceIdType.MESH,
        )

    for one, other in zip(backward, pieces):
        by_y(*other).start()
        by_x(*one).start()
        if other[0] < RING_OWN:
            @pl.when(jnp.logical_and(end, feeds_near))
            def _():
                by_ring(*other).start()

        if other[0] in STRAIGHT:
            @pl.when(jnp.logical_and(end, feeds_near))
            def _():
                fourth_straight(*other).start()

    for copy in weight_copies:
        copy.start()
    incident_copy.start()
    near_copy.start()

    def pass_greeting():
        @pl.when(jnp.logical_not(first))
        def _():
            pl.semaphore_wait(chain_sem, 1)

        @pl.when(jnp.logical_not(last))
        def _():
            greet(chain_sem, panel=to_z)

    @pl.when(jnp.logical_and(y == 1, at_chain <= 1))
    def _():
        pass_greeting()

    for copy in scalar_copies:
        copy.wait()
    live = counts_ref[0, 0]
    readers = partial_value.shape[0]
    steps_of = (0, 1 - 2 * x, 2 * way, -2 * way, 2 * x - 1)
    chosen = []
    for steps in steps_of:
        row = []
        for slot in range(slots):
            index, found, reader = 0, 0, 0
            for k in range(count):
                hit = jnp.logical_and(
                    jnp.logical_and(
                        pairs_ref[0, 0, 0, k] == reach + steps, pairs_ref[0, 1, 0, k] == slot
                    ),
                    k < live,
                )
                index = jnp.where(hit, k, index)
                found = jnp.where(hit, 1, found)
                reader = jnp.where(hit, pairs_ref[0, 2, 0, k], reader)
            block = send_ref[0, reach + steps, slot, panel(steps)]
            row.append((index, found, reader, block))
        chosen.append(row)
    for copy in weight_copies:
        copy.wait()

    def product(terms, at):
        left, right = [], []
        for place, part in terms:
            for index, found, reader, block in chosen[place]:
                left.append(weights[index, at, part * piece:(part + 1) * piece])
                value = windows[part][place, 0]
                for b in range(1, blocks):
                    value = jnp.where(block == b, windows[part][place, b], value)
                right.append(
                    jnp.concatenate(
                        [
                            jnp.where(
                                jnp.logical_and(found == 1, reader == r),
                                value, jnp.zeros_like(value),
                            )
                            for r in range(readers)
                        ],
                        axis=1,
                    )
                )
        return jnp.dot(
            jnp.concatenate(left, axis=1), jnp.concatenate(right, axis=0),
            preferred_element_type=jnp.float32,
        )

    rows = depth // CHUNKS
    chunks = [slice(chunk * rows, (chunk + 1) * rows) for chunk in range(CHUNKS)]

    def add(*terms, fresh=False):
        for at in chunks:
            term = product(terms, at)
            running[at, :] = term if fresh else running[at, :] + term

    add(*[(OWN, part) for part in range(PARTS)], fresh=True)

    for step in range(len(pieces) + max(ASIDE, BEHIND)):
        if step < len(pieces):
            part, block = pieces[step]

            @pl.when(end)
            def _():
                if backward[step][0] >= alone:
                    landing(ACROSS, *backward[step]).wait_recv()
                if backward[step][0] >= DIRECT and backward[step][0] not in STRAIGHT:
                    @pl.when(feeds_far)
                    def _():
                        fourth_by_ring(*backward[step]).start()

            landing(BESIDE, part, block).wait_recv()
            if part < DIRECT:
                @pl.when(skips_z)
                def _():
                    fourth_at_once(part, block).start()

            if step < LATE_GREETING:
                @pl.when(
                    jnp.logical_not(
                        jnp.logical_or(waits_long, skips_z) if part < RING_OWN else waits_long
                    )
                )
                def _():
                    by_z(part, block).start()
            else:
                if step == LATE_GREETING:
                    @pl.when(waits_long)
                    def _():
                        pass_greeting()
                        for missed in pieces[:step]:
                            by_z(*missed).start()

                @pl.when(jnp.logical_not(skips_z) if part < RING_OWN else here >= 0)
                def _():
                    by_z(part, block).start()

            @pl.when(feeds_near if part < NEAR_BY_X else near_end)
            def _():
                fourth_by_x(part, block).start()

        if ASIDE <= step < len(pieces) + ASIDE:
            turn = step - ASIDE
            part, block = backward[turn]

            @pl.when(jnp.logical_not(end))
            def _():
                if part >= alone:
                    landing(ACROSS, part, block).wait_recv()
                if part >= NEAR_BY_X:
                    @pl.when(jnp.logical_and(feeds_near, jnp.logical_not(first)))
                    def _():
                        fourth_by_y(part, block).start()

                if part >= FAR_BY_X:
                    @pl.when(feeds_far)
                    def _():
                        fourth_by_y(part, block).start()

            if turn % blocks == blocks - 1:
                add((BESIDE, turn // blocks))
        if step == 1:
            @pl.when(jnp.logical_and(y == 1, jnp.logical_and(at_chain > 1, jnp.logical_not(last))))
            def _():
                pass_greeting()
        if BEHIND <= step < len(pieces) + BEHIND:
            part, block = pieces[step - BEHIND]

            @pl.when(jnp.logical_and(feeds_far, jnp.logical_not(first)))
            def _():
                landing(BEYOND, part, block).wait_recv()
                if part < FAR_BY_X:
                    fourth_by_x(part, block).start()

    @pl.when(jnp.logical_and(feeds_near, jnp.logical_not(before_end)))
    def _():
        for part, block in backward:
            if part >= FAR_BY_X:
                landing(TRANSIT, part, block).wait_recv()
                fourth_by_z(part, block).start()

    def arrive(place, part):
        if place == BEYOND:
            @pl.when(jnp.logical_or(feeds_near, first))
            def _():
                for block in range(blocks):
                    landing(place, part, block).wait_recv()

            if part < FAR_BY_X:
                @pl.when(jnp.logical_and(end, feeds_far))
                def _():
                    for block in range(blocks):
                        fourth_by_x(part, block).start()
        else:
            bulk(blocks, 0, arrival(FOURTH, part, 0)).wait_recv()

    bulk(alone * blocks, 0, arrival(ACROSS, 0, 0)).wait_recv()
    add(*[(ACROSS, part) for part in range(PARTS)])
    order = [(BEYOND, 0)]
    for part in range(1, PARTS):
        order += [(BEYOND, part), (FOURTH, part - 1)]
    order.append((FOURTH, PARTS - 1))
    for place, part in order[:-1]:
        arrive(place, part)
        add((place, part))
    incident_copy.wait()
    near_copy.wait()
    arrive(*order[-1])
    sums = []
    for chunk, at in enumerate(chunks):
        total = running[at, :] + product(order[-1:], at)
        for r in range(readers):
            partial_value[r, at, :] = total[:, r * fields:(r + 1) * fields]
        for ahead in range(1, lags):
            other = lax.rem(lag + ahead, lags)
            copy = pltpu.make_async_remote_copy(
                src_ref=partial_value.at[pl.ds(other * own, own), pl.ds(chunk * rows, rows)],
                dst_ref=landed.at[ahead - 1, :, pl.ds(chunk * rows, rows)],
                send_sem=sum_send_sem.at[ahead - 1],
                recv_sem=sum_recv_sem.at[ahead - 1, chunk],
                device_id={"lag": other},
                device_id_type=pl.DeviceIdType.MESH,
            )
            copy.start()
            sums.append(copy)
    def parts_of(taken):
        return blocks * len([part for part in range(PARTS) if taken(part)])

    def when(condition, number):
        return jnp.where(condition, number, 0).astype(jnp.int32)

    near_x, far_x = NEAR_BY_X * blocks, FAR_BY_X * blocks
    ringed, at_once = RING_OWN * blocks, DIRECT * blocks
    straight = parts_of(lambda part: part in STRAIGHT)
    extra = jnp.where(
        feeds_near,
        near_x
        + when(near_end, each - near_x)
        + when(jnp.logical_not(first), each - near_x)
        + when(jnp.logical_not(before_end), each - far_x)
        + when(end, ringed + straight),
        when(jnp.logical_not(first), far_x)
        + when(jnp.logical_not(end), each - far_x)
        + when(end, far_x + each - straight - at_once)
        + when(before_end, at_once),
    )

    @pl.when(skips_z)
    def _():
        bulk(3 * each - ringed, 0, 0).wait_send()

    @pl.when(jnp.logical_not(skips_z))
    def _():
        bulk(3 * each, 0, 0).wait_send()

    for number in range(blocks, 3 * each, blocks):
        @pl.when(extra == number)
        def _():
            bulk(number, 1, 0).wait_send()

    solved = [None] * own
    for chunk, at in enumerate(chunks):
        for copy in sums[chunk * (lags - 1):(chunk + 1) * (lags - 1)]:
            copy.wait_recv()
        for j in range(own):
            summed = partial_value[lag * own + j, at]
            for ahead in range(1, lags):
                summed = summed + landed[ahead - 1, j, at]
            remainder = (incident[j, at].astype(jnp.float32) - summed).astype(jnp.bfloat16)
            term = jnp.dot(near[j, :, at], remainder, preferred_element_type=jnp.float32)
            solved[j] = term if chunk == 0 else solved[j] + term
    for j in range(own):
        out_ref[j] = solved[j].astype(out_ref.dtype)
    for ahead in range(1, lags):
        whole = partial_value.at[pl.ds(0, own)]
        pltpu.make_async_remote_copy(
            src_ref=whole, dst_ref=whole,
            send_sem=sum_send_sem.at[ahead - 1], recv_sem=sum_recv_sem.at[ahead - 1, 0],
            device_id={"lag": lax.rem(lag + ahead, lags)},
            device_id_type=pl.DeviceIdType.MESH,
        ).wait_send()


def relayed(panels, lags, history, weights, pairs, counts, send_list, incident, near_inverse):
    readers, depth, fields = history.shape[1:]
    count = weights.shape[2]
    own = incident.shape[0]
    piece = depth // PARTS
    arrivals = PARTS * (2 * readers + 1) + 1 + readers * (
        2 * PARTS - min(NEAR_BY_X, FAR_BY_X) - FAR_BY_X
    )
    in_hbm = pl.BlockSpec(memory_space=pltpu.HBM)
    dma = pltpu.SemaphoreType.DMA
    held = [
        pltpu.with_memory_space_constraint(operand, pltpu.HBM)
        for operand in (
            jnp.transpose(pairs, (0, 3, 1, 2)), jnp.transpose(send_list, (1, 2, 3, 0)),
            history, weights, incident, near_inverse,
        )
    ]
    return pl.pallas_call(
        functools.partial(relay_kernel, panels, lags),
        out_shape=pltpu.VMEM(incident.shape, jnp.bfloat16),
        in_specs=[pl.BlockSpec(memory_space=pltpu.SMEM)] + [in_hbm] * 6,
        out_specs=pl.BlockSpec(memory_space=pltpu.VMEM),
        scratch_shapes=[
            *[pltpu.SMEM(operand.shape, operand.dtype) for operand in held[:2]],
            dma((2,)),
            [pltpu.VMEM((TRANSIT + 1, readers, piece, fields), history.dtype)] * PARTS,
            pltpu.VMEM(weights.shape[2:], weights.dtype),
            pltpu.VMEM(near_inverse.shape, near_inverse.dtype),
            pltpu.VMEM(incident.shape, incident.dtype),
            pltpu.VMEM((depth, readers * fields), jnp.float32),
            pltpu.VMEM((readers, depth, fields), jnp.float32),
            pltpu.VMEM((lags - 1, own, depth, fields), jnp.float32),
            dma((2,)),
            dma((arrivals,)),
            dma,
            dma,
            dma,
            dma,
            dma((lags - 1,)),
            dma((lags - 1, CHUNKS)),
            pltpu.SemaphoreType.REGULAR,
        ],
        compiler_params=pltpu.CompilerParams(
            collective_id=0, has_side_effects=True, vmem_limit_bytes=48 * 1024 * 1024
        ),
    )(counts, *held)


def step_kernel(
    relay, panels, lags,
    pairs_ref, counts_ref, send_ref, local_ref, weights_ref, incident_ref, near_ref,
    out_ref,
    windows, weights, near, incident, right, running, partial_value, landed,
    send_sem, recv_sem, local_sem, weight_sem, near_sem, incident_sem,
    sum_send_sem, sum_recv_sem,
):
    here = lax.axis_index("panel")
    lag = lax.axis_index("lag")
    offsets = send_ref.shape[1]
    reach = offsets // 2
    blocks, piece, fields = windows[0].shape[1:]
    depth = piece * PARTS
    count = weights.shape[0]
    own = incident.shape[0]
    side = 2 * lax.rem(here, 2) - 1

    def panel(steps):
        return lax.rem(here + steps + panels, panels)

    def rows_of(part):
        return pl.ds(part * piece, piece)

    def outgoing(steps, part):
        if relay:
            return windows[part].at[0]
        return local_ref.at[reach - steps, :, rows_of(part)]

    source_here = local_ref.at[0] if relay else local_ref.at[reach]
    locals_here = [
        pltpu.make_async_copy(
            source_here.at[:, rows_of(part)], windows[part].at[0], local_sem.at[part]
        )
        for part in range(PARTS)
    ]
    for copy in locals_here:
        copy.start()
    weight_copies = [
        pltpu.make_async_copy(weights_ref.at[0, 0, k], weights.at[k], weight_sem.at[k])
        for k in range(count)
    ]

    barrier = pltpu.get_barrier_semaphore()
    greeted = [-side, 2 * side, -2 * side] + ([] if relay else [side])
    for steps in greeted:
        pl.semaphore_signal(
            barrier, inc=1, device_id={"panel": panel(steps)},
            device_id_type=pl.DeviceIdType.MESH,
        )
    for ahead in range(1, lags):
        pl.semaphore_signal(
            barrier, inc=1, device_id={"lag": lax.rem(lag + ahead, lags)},
            device_id_type=pl.DeviceIdType.MESH,
        )
    pl.semaphore_wait(barrier, len(greeted) + lags - 1)
    for copy in locals_here:
        copy.wait()

    def send(source, slot, part, steps):
        copy = pltpu.make_async_remote_copy(
            src_ref=source,
            dst_ref=windows[part].at[slot],
            send_sem=send_sem.at[slot - 1, part],
            recv_sem=recv_sem.at[slot - 1, part],
            device_id={"panel": panel(steps)},
            device_id_type=pl.DeviceIdType.MESH,
        )
        copy.start()
        return copy

    first, second, partner, passed = [], [], [], []
    lead = PARTS // 2
    for step in range(PARTS + lead):
        if step < PARTS:
            first.append(send(outgoing(2 * side, step), 3, step, 2 * side))
            partner.append(send(outgoing(-side, step), 4, step, -side))
        if step >= lead:
            part = step - lead
            second.append(send(outgoing(-2 * side, part), 2, part, -2 * side))
    near_copy = pltpu.make_async_copy(near_ref, near, near_sem)
    incident_copy = pltpu.make_async_copy(incident_ref, incident, incident_sem)
    for copy in weight_copies:
        copy.start()
    incident_copy.start()
    near_copy.start()
    def pass_on(part):
        if relay:
            first[part].wait_recv()
            passed.append(send(windows[part].at[3], 1, part, -side))
        else:
            passed.append(send(outgoing(side, part), 1, part, side))

    for part in range(PARTS):
        pass_on(part)
    for copy in weight_copies:
        copy.wait()
    incident_copy.wait()
    near_copy.wait()

    live = counts_ref[0, 0]
    readers = right.shape[2] // fields
    chosen = []
    for k in range(count):
        offset = pairs_ref[0, 0, 0, k]
        slot = pairs_ref[0, 1, 0, k]
        reader = pairs_ref[0, 2, 0, k]
        if relay:
            block = send_ref[0, offset, slot, panel(offset - reach)]
        else:
            block = slot
        place = lax.rem((offset - reach) * side + offsets, offsets)
        chosen.append((place, block, reader))

    def arrive(part):
        if not relay:
            first[part].wait_recv()
        partner[part].wait_recv()
        second[part].wait_recv()
        passed[part].wait_recv()
        for k, (place, block, reader) in enumerate(chosen):
            value = windows[part][place, block]
            for r in range(readers):
                kept = jnp.logical_and(reader == r, k < live)
                right[part, k * piece:(k + 1) * piece, r * fields:(r + 1) * fields] = jnp.where(
                    kept, value, jnp.zeros_like(value)
                )

    def product(part, at):
        left = jnp.concatenate(
            [weights[k, at, part * piece:(part + 1) * piece] for k in range(count)], axis=1
        )
        return jnp.dot(left, right[part], preferred_element_type=jnp.float32)

    rows = depth // CHUNKS
    sums = []
    for part in range(PARTS - 1):
        arrive(part)
        for chunk in range(CHUNKS):
            at = slice(chunk * rows, (chunk + 1) * rows)
            term = product(part, at)
            running[at, :] = term if part == 0 else running[at, :] + term
    arrive(PARTS - 1)
    for chunk in range(CHUNKS):
        at = slice(chunk * rows, (chunk + 1) * rows)
        total = running[at, :] + product(PARTS - 1, at)
        for r in range(readers):
            partial_value[r, at, :] = total[:, r * fields:(r + 1) * fields]
        for ahead in range(1, lags):
            other = lax.rem(lag + ahead, lags)
            copy = pltpu.make_async_remote_copy(
                src_ref=partial_value.at[pl.ds(other * own, own), pl.ds(chunk * rows, rows)],
                dst_ref=landed.at[ahead - 1, :, pl.ds(chunk * rows, rows)],
                send_sem=sum_send_sem.at[ahead - 1, chunk],
                recv_sem=sum_recv_sem.at[ahead - 1, chunk],
                device_id={"lag": other},
                device_id_type=pl.DeviceIdType.MESH,
            )
            copy.start()
            sums.append(copy)
    for copy in first + partner + second + passed:
        copy.wait_send()
    for copy in sums:
        copy.wait_recv()
    for j in range(own):
        summed = partial_value[lag * own + j]
        for ahead in range(1, lags):
            summed = summed + landed[ahead - 1, j]
        remainder = (incident[j].astype(jnp.float32) - summed).astype(jnp.bfloat16)
        out_ref[j] = jnp.dot(
            near[j], remainder, preferred_element_type=jnp.float32
        ).astype(out_ref.dtype)
    for copy in sums:
        copy.wait_send()


def on_device(panels, lags, history, weights, pairs, counts, send_list, incident, near_inverse):
    readers, depth, fields = history.shape[1:]
    offsets, slots = send_list.shape[2:]
    assert offsets == 5 and panels % 2 == 0 and panels > offsets
    count = weights.shape[2]
    own = incident.shape[0]
    if readers <= slots and panels % 4 == 0 and panels > 8:
        return relayed(
            panels, lags, history, weights, pairs, counts, send_list, incident, near_inverse
        )
    relay = readers <= slots
    blocks = readers if relay else slots
    local = history
    if not relay:
        here = lax.axis_index("panel")
        mine = lax.dynamic_index_in_dim(send_list, here, 0, keepdims=False)[0]
        local = jnp.take(history[0], mine.reshape(-1), axis=0).reshape(
            (offsets, slots, depth, fields)
        )
    anywhere = pl.BlockSpec(memory_space=pl.ANY)
    scalars = pl.BlockSpec(memory_space=pltpu.SMEM)
    dma = pltpu.SemaphoreType.DMA
    return pl.pallas_call(
        functools.partial(step_kernel, relay, panels, lags),
        out_shape=jax.ShapeDtypeStruct(incident.shape, jnp.bfloat16),
        in_specs=[scalars] * 3 + [anywhere] * 4,
        out_specs=pl.BlockSpec(memory_space=pltpu.VMEM),
        scratch_shapes=[
            [pltpu.VMEM((offsets, blocks, depth // PARTS, fields), history.dtype)] * PARTS,
            pltpu.VMEM(weights.shape[2:], weights.dtype),
            pltpu.VMEM(near_inverse.shape, near_inverse.dtype),
            pltpu.VMEM(incident.shape, incident.dtype),
            pltpu.VMEM((PARTS, count * depth // PARTS, readers * fields), history.dtype),
            pltpu.VMEM((depth, readers * fields), jnp.float32),
            pltpu.VMEM((readers, depth, fields), jnp.float32),
            pltpu.VMEM((lags - 1, own, depth, fields), jnp.float32),
            dma((offsets - 1, PARTS)),
            dma((offsets - 1, PARTS)),
            dma((PARTS,)),
            dma((count,)),
            dma,
            dma,
            dma((lags - 1, CHUNKS)),
            dma((lags - 1, CHUNKS)),
        ],
        compiler_params=pltpu.CompilerParams(
            collective_id=0, has_side_effects=True, vmem_limit_bytes=67043328
        ),
    )(jnp.transpose(pairs, (0, 3, 1, 2)), counts, jnp.transpose(send_list, (1, 2, 3, 0)), local, weights, incident, near_inverse)


def solution(mesh):
    return jax.shard_map(
        functools.partial(on_device, mesh.shape["panel"], mesh.shape["lag"]),
        mesh=mesh,
        in_specs=(
            P("lag", "panel", None, None),
            P("panel", "lag", None, None, None),
            P("panel", "lag", None, None),
            P("panel", "lag"),
            P(None, "lag", None, None),
            P(("panel", "lag"), None, None),
            P(("panel", "lag"), None, None),
        ),
        out_specs=P(("panel", "lag"), None, None),
        check_vma=False,
    )
```

```python
import functools

import jax
import jax.numpy as jnp
from jax import lax
from jax.experimental import pallas as pl
from jax.experimental.pallas import tpu as pltpu
from jax.sharding import PartitionSpec as P

CHUNKS = 2
PARTS = 4

NEAR_BY_X = 2
FAR_BY_X = 3
RING = (2,)
RING_FAR = ()
AT_ONCE = (0,)
STRAIGHT = (1,)
HANDED = (3,)
RING_STEP = 5
DEFERRED = 2
SPLIT = 1
OWN, ACROSS, BESIDE, BEYOND, FOURTH, TRANSIT, LASTING = range(7)
BEHIND = 5
ASIDE = 3
LATE_GREETING = 3


def relay_kernel(
    panels, lags,
    counts_ref, pairs_hbm, send_hbm, local_ref, weights_ref, incident_ref, near_ref,
    out_ref,
    pairs_ref, send_ref, scalar_sem,
    windows, weights, near, incident, running, theirs, mine, landed,
    send_sem, recv_sem, local_sem, weight_sem, near_sem, incident_sem,
    sum_send_sem, sum_recv_sem, chain_sem,
):
    here = lax.axis_index("panel")
    lag = lax.axis_index("lag")
    offsets, slots = send_ref.shape[1:3]
    reach = offsets // 2
    subs, small, fields = windows[0].shape[1:]
    blocks = subs // SPLIT
    piece = small * SPLIT
    depth = piece * PARTS
    count = weights.shape[0]
    own = incident.shape[0]
    places = panels // 4
    x = lax.rem(here, 2)
    y = lax.rem(here // 2, 2)
    way = 1 - 2 * y
    z = here // 4
    at_chain = jnp.where(y == 0, z, places - 1 - z)
    first = at_chain == 0
    last = at_chain == places - 1
    feeds_near = x == y
    feeds_far = x != y
    start = jnp.logical_and(y == 0, first)
    before_end = jnp.logical_and(y == 0, last)
    end = jnp.logical_and(y == 1, first)
    waits_long = jnp.logical_and(y == 1, last)
    near_end = jnp.logical_and(feeds_near, jnp.logical_or(before_end, start))
    near_aside = jnp.logical_and(
        feeds_near, jnp.logical_not(jnp.logical_or(end, waits_long))
    )
    skips_z = jnp.logical_and(before_end, feeds_far)
    skips_far = jnp.logical_and(before_end, feeds_near)
    start_far = jnp.logical_and(start, feeds_far)

    def stays(part, block):
        skipped = here < 0
        if part in RING or (part, block) in deferred:
            skipped = jnp.logical_or(skipped, skips_z)
        if part in RING_FAR:
            skipped = jnp.logical_or(skipped, skips_far)
        return skipped


    def panel(steps):
        return lax.rem(here + steps + panels, panels)

    to_x = panel(1 - 2 * x)
    to_y = panel(2 * way)
    to_z = panel(4 * way)
    from_z = panel(-4 * way)
    to_start = panel(2)
    to_first = panel(3)

    locals_here = [
        pltpu.make_async_copy(
            local_ref.at[0, sub // SPLIT, pl.ds(part * piece + sub % SPLIT * small, small)],
            windows[part].at[OWN, sub],
            local_sem,
        )
        for part in range(PARTS)
        for sub in range(subs)
    ]
    for copy in locals_here:
        copy.start()
    scalar_copies = [
        pltpu.make_async_copy(source, target, scalar_sem.at[i])
        for i, (source, target) in enumerate([(pairs_hbm, pairs_ref), (send_hbm, send_ref)])
    ]
    for copy in scalar_copies:
        copy.start()
    weight_copies = [
        pltpu.make_async_copy(weights_ref.at[0, 0], weights, weight_sem)
    ]
    near_copy = pltpu.make_async_copy(near_ref, near, near_sem)
    incident_copy = pltpu.make_async_copy(incident_ref, incident, incident_sem)

    barrier = pltpu.get_barrier_semaphore()

    def greet(semaphore, **device):
        pl.semaphore_signal(
            semaphore, inc=1, device_id=device, device_id_type=pl.DeviceIdType.MESH
        )

    greet(barrier, panel=to_x)
    greet(barrier, panel=to_y)

    @pl.when(jnp.logical_not(end))
    def _():
        greet(barrier, panel=from_z)

    @pl.when(start)
    def _():
        greet(barrier, panel=panel(-2))

        @pl.when(feeds_near)
        def _():
            greet(barrier, panel=panel(-3))
            greet(barrier, panel=panel(-1))

    for ahead in range(1, lags):
        greet(barrier, lag=lax.rem(lag + ahead, lags))
    pl.semaphore_wait(
        barrier,
        1
        + lags
        + jnp.where(
            waits_long, 0,
            jnp.where(end, jnp.where(feeds_near, 3, 2), jnp.where(skips_z, 2, 1)),
        ).astype(jnp.int32),
    )
    pltpu.make_async_copy(local_ref.at[0], local_ref.at[0], local_sem).wait()

    pieces = [(part, sub) for part in range(PARTS) for sub in range(subs)]
    backward = pieces[::-1]

    alone = min(NEAR_BY_X, FAR_BY_X)
    each = PARTS * subs
    relayed_across = (PARTS - alone) * subs

    def arrival(target, part, block):
        if target == BESIDE:
            return part * subs + block
        if target == BEYOND:
            return each + part * subs + block
        if target == ACROSS:
            place = (part - alone) * subs + block if part >= alone else relayed_across
            return 2 * each + place
        if target == FOURTH:
            return 2 * each + relayed_across + 1 + part
        return 2 * each + relayed_across + 1 + PARTS + (part - FAR_BY_X) * subs + block

    def copy_of(source, target, link, part, block, device, lands=None):
        return pltpu.make_async_remote_copy(
            src_ref=windows[part].at[source, block],
            dst_ref=windows[part].at[target, block],
            send_sem=send_sem.at[link],
            recv_sem=recv_sem.at[arrival(target, part, block) if lands is None else lands],
            device_id={"panel": device},
            device_id_type=pl.DeviceIdType.MESH,
        )

    def by_x(part, block):
        return copy_of(OWN, ACROSS, 0, part, block, to_x)

    def by_y(part, block):
        return copy_of(OWN, BESIDE, 0, part, block, to_y)

    def by_z(part, block):
        return copy_of(BESIDE, BEYOND, 0, part, block, to_z)

    def fourth_by_x(part, block):
        return copy_of(jnp.where(feeds_near, BESIDE, BEYOND), FOURTH, 1, part, block, to_x)

    def fourth_by_y(part, block):
        if part < FAR_BY_X:
            return copy_of(ACROSS, FOURTH, 1, part, block, to_y)
        lands = jnp.where(
            feeds_near, arrival(FOURTH, part, block), arrival(TRANSIT, part, block)
        )
        return copy_of(
            ACROSS, jnp.where(feeds_near, FOURTH, TRANSIT), 1, part, block, to_y, lands
        )

    def fourth_by_z(part, block):
        return copy_of(TRANSIT, FOURTH, 1, part, block, to_z)

    def by_ring(part, block):
        return copy_of(OWN, BEYOND, 1, part, block, to_start)

    def fourth_by_ring(part, block):
        return copy_of(ACROSS, FOURTH, 1, part, block, to_start)

    def fourth_at_once(part, block):
        return copy_of(BESIDE, FOURTH, 1, part, block, to_first)

    def fourth_straight(part, block):
        return copy_of(OWN, FOURTH, 1, part, block, panel(1))

    def landing(slot, part, block):
        return copy_of(slot, slot, 0, part, block, to_x)

    def bulk(number, link, lands):
        rows = number * small * fields // (2 * weights.shape[2])
        stretch = weights.at[pl.ds(0, 2), pl.ds(0, rows)]
        return pltpu.make_async_remote_copy(
            src_ref=stretch, dst_ref=stretch,
            send_sem=send_sem.at[link], recv_sem=recv_sem.at[lands],
            device_id={"panel": to_x}, device_id_type=pl.DeviceIdType.MESH,
        )

    for one, other in zip(backward, pieces):
        by_y(*other).start()
        by_x(*one).start()
        if other[0] in RING:
            @pl.when(jnp.logical_and(end, feeds_near))
            def _():
                by_ring(*other).start()

        if other[0] in RING_FAR:
            @pl.when(jnp.logical_and(end, feeds_far))
            def _():
                by_ring(*other).start()

        if other[0] in STRAIGHT:
            @pl.when(jnp.logical_and(end, feeds_near))
            def _():
                fourth_straight(*other).start()

    for copy in weight_copies:
        copy.start()
    incident_copy.start()
    near_copy.start()

    def pass_greeting():
        @pl.when(jnp.logical_not(first))
        def _():
            pl.semaphore_wait(chain_sem, 1)

        @pl.when(jnp.logical_not(last))
        def _():
            greet(chain_sem, panel=to_z)

    @pl.when(jnp.logical_and(y == 1, at_chain <= 1))
    def _():
        pass_greeting()

    for copy in scalar_copies:
        copy.wait()
    live = counts_ref[0, 0]
    readers = running.shape[0]
    steps_of = (0, 1 - 2 * x, 2 * way, -2 * way, 2 * x - 1)
    chosen = []
    for steps in steps_of:
        row = []
        for slot in range(slots):
            index, found, reader = 0, 0, 0
            for k in range(count):
                hit = jnp.logical_and(
                    jnp.logical_and(
                        pairs_ref[0, 0, 0, k] == reach + steps, pairs_ref[0, 1, 0, k] == slot
                    ),
                    k < live,
                )
                index = jnp.where(hit, k, index)
                found = jnp.where(hit, 1, found)
                reader = jnp.where(hit, pairs_ref[0, 2, 0, k], reader)
            block = send_ref[0, reach + steps, slot, panel(steps)]
            row.append((index, found, reader, block))
        chosen.append(row)
    for copy in weight_copies:
        copy.wait()

    z_last = jnp.logical_and(start, feeds_near)
    lasting_place = (jnp.where(z_last, FOURTH, BEYOND), jnp.where(z_last, BEYOND, FOURTH))
    pairs_of = list(zip(chosen[FOURTH], chosen[BEYOND]))
    lasting = (
        [[jnp.where(z_last, f, b) for f, b in zip(*both)] for both in pairs_of],
        [[jnp.where(z_last, b, f) for f, b in zip(*both)] for both in pairs_of],
    )

    def block_of(part, place, b):
        return windows[part][place, b * SPLIT:(b + 1) * SPLIT].reshape((piece, fields))

    def product(terms, at, columns):
        left, right = [], []
        for place, part in terms:
            entries = chosen[place] if place < LASTING else lasting[place - LASTING]
            place = place if place < LASTING else lasting_place[place - LASTING]
            for index, found, reader, block in entries:
                left.append(weights[index, at, part * piece:(part + 1) * piece])
                value = block_of(part, place, 0)
                for b in range(1, blocks):
                    value = jnp.where(block == b, block_of(part, place, b), value)
                kept = [
                    jnp.where(
                        jnp.logical_and(found == 1, reader == r), value, jnp.zeros_like(value)
                    )
                    for r in columns
                ]
                right.append(jnp.concatenate(kept, axis=1))
        return jnp.dot(
            jnp.concatenate(left, axis=1), jnp.concatenate(right, axis=0),
            preferred_element_type=jnp.float32,
        )

    rows = depth // CHUNKS
    chunks = [slice(chunk * rows, (chunk + 1) * rows) for chunk in range(CHUNKS)]

    def add(*terms, fresh=False):
        for at in chunks:
            term = product(terms, at, range(readers))
            for r in range(readers):
                column = term[:, r * fields:(r + 1) * fields]
                running[r, at] = column if fresh else running[r, at] + column

    add(*[(OWN, part) for part in range(PARTS)], fresh=True)

    deferred = [(part, block) for part, block in pieces if part in AT_ONCE][:DEFERRED]

    for step in range(len(pieces) + max(ASIDE, BEHIND)):
        if step < len(pieces):
            part, block = pieces[step]

            @pl.when(end)
            def _():
                if backward[step][0] >= alone:
                    landing(ACROSS, *backward[step]).wait_recv()
                if backward[step][0] in HANDED:
                    @pl.when(feeds_far)
                    def _():
                        fourth_by_ring(*backward[step]).start()

            landing(BESIDE, part, block).wait_recv()
            if part in AT_ONCE:
                @pl.when(skips_z)
                def _():
                    fourth_at_once(part, block).start()

            if step < LATE_GREETING:
                @pl.when(jnp.logical_not(jnp.logical_or(waits_long, stays(part, block))))
                def _():
                    by_z(part, block).start()
            else:
                if step == LATE_GREETING:
                    @pl.when(waits_long)
                    def _():
                        pass_greeting()
                        for missed in pieces[:step]:
                            by_z(*missed).start()

                @pl.when(jnp.logical_not(stays(part, block)))
                def _():
                    by_z(part, block).start()

            if deferred and (part, block) == deferred[-1]:
                @pl.when(skips_z)
                def _():
                    for missed in deferred:
                        by_z(*missed).start()

            if step == RING_STEP:
                @pl.when(start_far)
                def _():
                    for ring_part, ring_block in pieces:
                        if ring_part in RING:
                            landing(BEYOND, ring_part, ring_block).wait_recv()
                            fourth_by_x(ring_part, ring_block).start()

            @pl.when(feeds_near if part < NEAR_BY_X else near_end)
            def _():
                fourth_by_x(part, block).start()

        if ASIDE <= step < len(pieces) + ASIDE:
            turn = step - ASIDE
            part, block = backward[turn]

            @pl.when(jnp.logical_not(end))
            def _():
                if part >= alone:
                    landing(ACROSS, part, block).wait_recv()
                if part >= NEAR_BY_X:
                    @pl.when(near_aside)
                    def _():
                        fourth_by_y(part, block).start()

                if part >= FAR_BY_X:
                    @pl.when(feeds_far)
                    def _():
                        fourth_by_y(part, block).start()

            if turn % subs == subs - 1:
                add((BESIDE, turn // subs))
        if step == 2 * SPLIT - 1:
            @pl.when(jnp.logical_and(y == 1, jnp.logical_and(at_chain > 1, jnp.logical_not(last))))
            def _():
                pass_greeting()
        if BEHIND <= step < len(pieces) + BEHIND:
            part, block = pieces[step - BEHIND]

            @pl.when(jnp.logical_and(feeds_far, jnp.logical_not(first)))
            def _():
                landing(BEYOND, part, block).wait_recv()
                if part < FAR_BY_X:
                    fourth_by_x(part, block).start()

        if step == len(pieces) - 1:
            bulk(alone * subs, 0, arrival(ACROSS, 0, 0)).wait_recv()
            add(*[(ACROSS, part) for part in range(alone)])
        if step == len(pieces) + ASIDE - 1:
            add(*[(ACROSS, part) for part in range(alone, PARTS)])

    @pl.when(jnp.logical_and(feeds_near, jnp.logical_not(before_end)))
    def _():
        for part, block in backward:
            if part >= FAR_BY_X:
                landing(TRANSIT, part, block).wait_recv()
                fourth_by_z(part, block).start()

    def arrive(place, part):
        if place >= LASTING:
            @pl.when(z_last if place == LASTING else jnp.logical_not(z_last))
            def _():
                arrive(FOURTH, part)

            @pl.when(z_last if place > LASTING else jnp.logical_not(z_last))
            def _():
                arrive(BEYOND, part)

            return
        if place == BEYOND:
            @pl.when(jnp.logical_or(feeds_near, end if part in RING else first))
            def _():
                for block in range(subs):
                    landing(place, part, block).wait_recv()

            if part < FAR_BY_X:
                @pl.when(jnp.logical_and(end, feeds_far))
                def _():
                    for block in range(subs):
                        fourth_by_x(part, block).start()
        else:
            bulk(subs, 0, arrival(FOURTH, part, 0)).wait_recv()

    order = [((BEYOND, 0), (BEYOND, 1))]
    order += [((FOURTH, part - 2), (BEYOND, part)) for part in range(2, PARTS - 1)]
    order += [((FOURTH, part),) for part in range(PARTS - 3, PARTS - 2)]
    order += [((FOURTH, PARTS - 2), (LASTING, PARTS - 1)), ((LASTING + 1, PARTS - 1),)]
    for group in order[:-1]:
        for place, part in group:
            arrive(place, part)
        add(*group)
    incident_copy.wait()
    near_copy.wait()
    arrive(*order[-1][0])
    sums = []
    for chunk, at in enumerate(chunks):
        for ahead in range(1, lags):
            other = lax.rem(lag + ahead, lags)
            for j in range(own):
                reader = other * own + j
                theirs[ahead - 1, j, at] = running[reader, at] + product(
                    order[-1], at, [reader]
                )
            copy = pltpu.make_async_remote_copy(
                src_ref=theirs.at[ahead - 1, :, pl.ds(chunk * rows, rows)],
                dst_ref=landed.at[ahead - 1, :, pl.ds(chunk * rows, rows)],
                send_sem=sum_send_sem.at[ahead - 1],
                recv_sem=sum_recv_sem.at[ahead - 1, chunk],
                device_id={"lag": other},
                device_id_type=pl.DeviceIdType.MESH,
            )
            copy.start()
            sums.append(copy)
    for at in chunks:
        for j in range(own):
            reader = lag * own + j
            mine[j, at] = incident[j, at].astype(jnp.float32) - (
                running[reader, at] + product(order[-1], at, [reader])
            )
    def parts_of(taken):
        return subs * len([part for part in range(PARTS) if taken(part)])

    def when(condition, number):
        return jnp.where(condition, number, 0).astype(jnp.int32)

    near_x, far_x = NEAR_BY_X * subs, FAR_BY_X * subs
    ringed = parts_of(lambda part: part in RING)
    ringed_far = parts_of(lambda part: part in RING_FAR)
    straight = parts_of(lambda part: part in STRAIGHT)
    at_once = parts_of(lambda part: part in AT_ONCE)
    handed = parts_of(lambda part: part in HANDED)
    extra = jnp.where(
        feeds_near,
        near_x
        + when(near_end, each - near_x)
        + when(near_aside, each - near_x)
        + when(jnp.logical_not(before_end), each - far_x)
        + when(end, ringed + straight),
        when(jnp.logical_not(first), far_x)
        + when(jnp.logical_not(end), each - far_x)
        + when(end, far_x + ringed_far + handed)
        + when(start, ringed)
        + when(before_end, at_once),
    )

    kept_back = when(skips_z, ringed) + when(skips_far, ringed_far)
    for number in sorted({0, ringed, ringed_far}):
        @pl.when(kept_back == number)
        def _():
            bulk(3 * each - number, 0, 0).wait_send()

    for number in range(subs, 3 * each, subs):
        @pl.when(extra == number)
        def _():
            bulk(number, 1, 0).wait_send()

    solved = [None] * own
    for chunk, at in enumerate(chunks):
        for copy in sums[chunk * (lags - 1):(chunk + 1) * (lags - 1)]:
            copy.wait_recv()
        for j in range(own):
            remainder = mine[j, at]
            for ahead in range(1, lags):
                remainder = remainder - landed[ahead - 1, j, at]
            remainder = remainder.astype(jnp.bfloat16)
            term = jnp.dot(near[j, :, at], remainder, preferred_element_type=jnp.float32)
            solved[j] = term if chunk == 0 else solved[j] + term
    for j in range(own):
        out_ref[j] = solved[j].astype(out_ref.dtype)
    for ahead in range(1, lags):
        whole = theirs.at[ahead - 1]
        pltpu.make_async_remote_copy(
            src_ref=whole, dst_ref=whole,
            send_sem=sum_send_sem.at[ahead - 1], recv_sem=sum_recv_sem.at[ahead - 1, 0],
            device_id={"lag": lax.rem(lag + ahead, lags)},
            device_id_type=pl.DeviceIdType.MESH,
        ).wait_send()


def relayed(panels, lags, history, weights, pairs, counts, send_list, incident, near_inverse):
    readers, depth, fields = history.shape[1:]
    count = weights.shape[2]
    own = incident.shape[0]
    piece = depth // PARTS
    subs = readers * SPLIT
    arrivals = PARTS * (2 * subs + 1) + 1 + subs * (
        2 * PARTS - min(NEAR_BY_X, FAR_BY_X) - FAR_BY_X
    )
    in_hbm = pl.BlockSpec(memory_space=pltpu.HBM)
    dma = pltpu.SemaphoreType.DMA
    held = [
        pltpu.with_memory_space_constraint(operand, pltpu.HBM)
        for operand in (
            jnp.transpose(pairs, (0, 3, 1, 2)), jnp.transpose(send_list, (1, 2, 3, 0)),
            history, weights, incident, near_inverse,
        )
    ]
    return pl.pallas_call(
        functools.partial(relay_kernel, panels, lags),
        out_shape=pltpu.VMEM(incident.shape, jnp.bfloat16),
        in_specs=[pl.BlockSpec(memory_space=pltpu.SMEM)] + [in_hbm] * 6,
        out_specs=pl.BlockSpec(memory_space=pltpu.VMEM),
        scratch_shapes=[
            *[pltpu.SMEM(operand.shape, operand.dtype) for operand in held[:2]],
            dma((2,)),
            [pltpu.VMEM((TRANSIT + 1, subs, piece // SPLIT, fields), history.dtype)] * PARTS,
            pltpu.VMEM(weights.shape[2:], weights.dtype),
            pltpu.VMEM(near_inverse.shape, near_inverse.dtype),
            pltpu.VMEM(incident.shape, incident.dtype),
            pltpu.VMEM((readers, depth, fields), jnp.float32),
            pltpu.VMEM((lags - 1, own, depth, fields), jnp.float32),
            pltpu.VMEM((own, depth, fields), jnp.float32),
            pltpu.VMEM((lags - 1, own, depth, fields), jnp.float32),
            dma((2,)),
            dma((arrivals,)),
            dma,
            dma,
            dma,
            dma,
            dma((lags - 1,)),
            dma((lags - 1, CHUNKS)),
            pltpu.SemaphoreType.REGULAR,
        ],
        compiler_params=pltpu.CompilerParams(
            collective_id=0, has_side_effects=True, vmem_limit_bytes=48 * 1024 * 1024
        ),
    )(counts, *held)


def step_kernel(
    relay, panels, lags,
    pairs_ref, counts_ref, send_ref, local_ref, weights_ref, incident_ref, near_ref,
    out_ref,
    windows, weights, near, incident, right, running, partial_value, landed,
    send_sem, recv_sem, local_sem, weight_sem, near_sem, incident_sem,
    sum_send_sem, sum_recv_sem,
):
    here = lax.axis_index("panel")
    lag = lax.axis_index("lag")
    offsets = send_ref.shape[1]
    reach = offsets // 2
    blocks, piece, fields = windows[0].shape[1:]
    depth = piece * PARTS
    count = weights.shape[0]
    own = incident.shape[0]
    side = 2 * lax.rem(here, 2) - 1

    def panel(steps):
        return lax.rem(here + steps + panels, panels)

    def rows_of(part):
        return pl.ds(part * piece, piece)

    def outgoing(steps, part):
        if relay:
            return windows[part].at[0]
        return local_ref.at[reach - steps, :, rows_of(part)]

    source_here = local_ref.at[0] if relay else local_ref.at[reach]
    locals_here = [
        pltpu.make_async_copy(
            source_here.at[:, rows_of(part)], windows[part].at[0], local_sem.at[part]
        )
        for part in range(PARTS)
    ]
    for copy in locals_here:
        copy.start()
    weight_copies = [
        pltpu.make_async_copy(weights_ref.at[0, 0, k], weights.at[k], weight_sem.at[k])
        for k in range(count)
    ]

    barrier = pltpu.get_barrier_semaphore()
    greeted = [-side, 2 * side, -2 * side] + ([] if relay else [side])
    for steps in greeted:
        pl.semaphore_signal(
            barrier, inc=1, device_id={"panel": panel(steps)},
            device_id_type=pl.DeviceIdType.MESH,
        )
    for ahead in range(1, lags):
        pl.semaphore_signal(
            barrier, inc=1, device_id={"lag": lax.rem(lag + ahead, lags)},
            device_id_type=pl.DeviceIdType.MESH,
        )
    pl.semaphore_wait(barrier, len(greeted) + lags - 1)
    for copy in locals_here:
        copy.wait()

    def send(source, slot, part, steps):
        copy = pltpu.make_async_remote_copy(
            src_ref=source,
            dst_ref=windows[part].at[slot],
            send_sem=send_sem.at[slot - 1, part],
            recv_sem=recv_sem.at[slot - 1, part],
            device_id={"panel": panel(steps)},
            device_id_type=pl.DeviceIdType.MESH,
        )
        copy.start()
        return copy

    first, second, partner, passed = [], [], [], []
    lead = PARTS // 2
    for step in range(PARTS + lead):
        if step < PARTS:
            first.append(send(outgoing(2 * side, step), 3, step, 2 * side))
            partner.append(send(outgoing(-side, step), 4, step, -side))
        if step >= lead:
            part = step - lead
            second.append(send(outgoing(-2 * side, part), 2, part, -2 * side))
    near_copy = pltpu.make_async_copy(near_ref, near, near_sem)
    incident_copy = pltpu.make_async_copy(incident_ref, incident, incident_sem)
    for copy in weight_copies:
        copy.start()
    incident_copy.start()
    near_copy.start()
    def pass_on(part):
        if relay:
            first[part].wait_recv()
            passed.append(send(windows[part].at[3], 1, part, -side))
        else:
            passed.append(send(outgoing(side, part), 1, part, side))

    for part in range(PARTS):
        pass_on(part)
    for copy in weight_copies:
        copy.wait()
    incident_copy.wait()
    near_copy.wait()

    live = counts_ref[0, 0]
    readers = right.shape[2] // fields
    chosen = []
    for k in range(count):
        offset = pairs_ref[0, 0, 0, k]
        slot = pairs_ref[0, 1, 0, k]
        reader = pairs_ref[0, 2, 0, k]
        if relay:
            block = send_ref[0, offset, slot, panel(offset - reach)]
        else:
            block = slot
        place = lax.rem((offset - reach) * side + offsets, offsets)
        chosen.append((place, block, reader))

    def arrive(part):
        if not relay:
            first[part].wait_recv()
        partner[part].wait_recv()
        second[part].wait_recv()
        passed[part].wait_recv()
        for k, (place, block, reader) in enumerate(chosen):
            value = windows[part][place, block]
            for r in range(readers):
                kept = jnp.logical_and(reader == r, k < live)
                right[part, k * piece:(k + 1) * piece, r * fields:(r + 1) * fields] = jnp.where(
                    kept, value, jnp.zeros_like(value)
                )

    def product(part, at):
        left = jnp.concatenate(
            [weights[k, at, part * piece:(part + 1) * piece] for k in range(count)], axis=1
        )
        return jnp.dot(left, right[part], preferred_element_type=jnp.float32)

    rows = depth // CHUNKS
    sums = []
    for part in range(PARTS - 1):
        arrive(part)
        for chunk in range(CHUNKS):
            at = slice(chunk * rows, (chunk + 1) * rows)
            term = product(part, at)
            running[at, :] = term if part == 0 else running[at, :] + term
    arrive(PARTS - 1)
    for chunk in range(CHUNKS):
        at = slice(chunk * rows, (chunk + 1) * rows)
        total = running[at, :] + product(PARTS - 1, at)
        for r in range(readers):
            partial_value[r, at, :] = total[:, r * fields:(r + 1) * fields]
        for ahead in range(1, lags):
            other = lax.rem(lag + ahead, lags)
            copy = pltpu.make_async_remote_copy(
                src_ref=partial_value.at[pl.ds(other * own, own), pl.ds(chunk * rows, rows)],
                dst_ref=landed.at[ahead - 1, :, pl.ds(chunk * rows, rows)],
                send_sem=sum_send_sem.at[ahead - 1, chunk],
                recv_sem=sum_recv_sem.at[ahead - 1, chunk],
                device_id={"lag": other},
                device_id_type=pl.DeviceIdType.MESH,
            )
            copy.start()
            sums.append(copy)
    for copy in first + partner + second + passed:
        copy.wait_send()
    for copy in sums:
        copy.wait_recv()
    for j in range(own):
        summed = partial_value[lag * own + j]
        for ahead in range(1, lags):
            summed = summed + landed[ahead - 1, j]
        remainder = (incident[j].astype(jnp.float32) - summed).astype(jnp.bfloat16)
        out_ref[j] = jnp.dot(
            near[j], remainder, preferred_element_type=jnp.float32
        ).astype(out_ref.dtype)
    for copy in sums:
        copy.wait_send()


def on_device(panels, lags, history, weights, pairs, counts, send_list, incident, near_inverse):
    readers, depth, fields = history.shape[1:]
    offsets, slots = send_list.shape[2:]
    assert offsets == 5 and panels % 2 == 0 and panels > offsets
    count = weights.shape[2]
    own = incident.shape[0]
    if readers <= slots and panels % 4 == 0 and panels > 8:
        return relayed(
            panels, lags, history, weights, pairs, counts, send_list, incident, near_inverse
        )
    relay = readers <= slots
    blocks = readers if relay else slots
    local = history
    if not relay:
        here = lax.axis_index("panel")
        mine = lax.dynamic_index_in_dim(send_list, here, 0, keepdims=False)[0]
        local = jnp.take(history[0], mine.reshape(-1), axis=0).reshape(
            (offsets, slots, depth, fields)
        )
    anywhere = pl.BlockSpec(memory_space=pl.ANY)
    scalars = pl.BlockSpec(memory_space=pltpu.SMEM)
    dma = pltpu.SemaphoreType.DMA
    return pl.pallas_call(
        functools.partial(step_kernel, relay, panels, lags),
        out_shape=jax.ShapeDtypeStruct(incident.shape, jnp.bfloat16),
        in_specs=[scalars] * 3 + [anywhere] * 4,
        out_specs=pl.BlockSpec(memory_space=pltpu.VMEM),
        scratch_shapes=[
            [pltpu.VMEM((offsets, blocks, depth // PARTS, fields), history.dtype)] * PARTS,
            pltpu.VMEM(weights.shape[2:], weights.dtype),
            pltpu.VMEM(near_inverse.shape, near_inverse.dtype),
            pltpu.VMEM(incident.shape, incident.dtype),
            pltpu.VMEM((PARTS, count * depth // PARTS, readers * fields), history.dtype),
            pltpu.VMEM((depth, readers * fields), jnp.float32),
            pltpu.VMEM((readers, depth, fields), jnp.float32),
            pltpu.VMEM((lags - 1, own, depth, fields), jnp.float32),
            dma((offsets - 1, PARTS)),
            dma((offsets - 1, PARTS)),
            dma((PARTS,)),
            dma((count,)),
            dma,
            dma,
            dma((lags - 1, CHUNKS)),
            dma((lags - 1, CHUNKS)),
        ],
        compiler_params=pltpu.CompilerParams(
            collective_id=0, has_side_effects=True, vmem_limit_bytes=67043328
        ),
    )(jnp.transpose(pairs, (0, 3, 1, 2)), counts, jnp.transpose(send_list, (1, 2, 3, 0)), local, weights, incident, near_inverse)


def solution(mesh):
    return jax.shard_map(
        functools.partial(on_device, mesh.shape["panel"], mesh.shape["lag"]),
        mesh=mesh,
        in_specs=(
            P("lag", "panel", None, None),
            P("panel", "lag", None, None, None),
            P("panel", "lag", None, None),
            P("panel", "lag"),
            P(None, "lag", None, None),
            P(("panel", "lag"), None, None),
            P(("panel", "lag"), None, None),
        ),
        out_specs=P(("panel", "lag"), None, None),
        check_vma=False,
    )
```

```python
import functools

import jax
import jax.numpy as jnp
from jax import lax
from jax.experimental import pallas as pl
from jax.experimental.pallas import tpu as pltpu
from jax.sharding import PartitionSpec as P

CHUNKS = 2
PARTS = 4

NEAR_BY_X = 2
FAR_BY_X = 3
RING = (2,)
RING_FAR = ()
AT_ONCE = (0,)
STRAIGHT = (1,)
HANDED = (3,)
RING_STEP = 5
GIVE_STEP = 2
DEFERRED = 2
SPLIT = 1
OWN, ACROSS, BESIDE, BEYOND, FOURTH, TRANSIT, LASTING = range(7)
BEHIND = 5
ASIDE = 3
LATE_GREETING = 3


def relay_kernel(
    panels, lags,
    counts_ref, pairs_hbm, send_hbm, local_ref, weights_ref, incident_ref, near_ref,
    out_ref,
    pairs_ref, send_ref, scalar_sem,
    windows, weights, near, incident, running, theirs, mine, landed,
    send_sem, recv_sem, local_sem, weight_sem, near_sem, incident_sem,
    sum_send_sem, sum_recv_sem, chain_sem, give_sem,
):
    here = lax.axis_index("panel")
    lag = lax.axis_index("lag")
    offsets, slots = send_ref.shape[1:3]
    reach = offsets // 2
    subs, small, fields = windows[0].shape[1:]
    blocks = subs // SPLIT
    piece = small * SPLIT
    depth = piece * PARTS
    count = weights.shape[0]
    own = incident.shape[0]
    places = panels // 4
    x = lax.rem(here, 2)
    y = lax.rem(here // 2, 2)
    way = 1 - 2 * y
    z = here // 4
    at_chain = jnp.where(y == 0, z, places - 1 - z)
    first = at_chain == 0
    last = at_chain == places - 1
    feeds_near = x == y
    feeds_far = x != y
    start = jnp.logical_and(y == 0, first)
    before_end = jnp.logical_and(y == 0, last)
    end = jnp.logical_and(y == 1, first)
    waits_long = jnp.logical_and(y == 1, last)
    near_end = jnp.logical_and(feeds_near, jnp.logical_or(before_end, start))
    near_aside = jnp.logical_and(
        feeds_near, jnp.logical_not(jnp.logical_or(end, waits_long))
    )
    skips_z = jnp.logical_and(before_end, feeds_far)
    skips_far = jnp.logical_and(before_end, feeds_near)
    start_far = jnp.logical_and(start, feeds_far)
    gives = jnp.logical_and(waits_long, feeds_near)
    takes = jnp.logical_and(jnp.logical_and(y == 0, at_chain == 1), feeds_near)
    far_aside = jnp.logical_and(feeds_far, jnp.logical_not(jnp.logical_or(end, waits_long)))
    far_over = jnp.logical_and(feeds_near, jnp.logical_not(jnp.logical_or(before_end, start)))

    def stays(part, block):
        skipped = here < 0
        if part in RING or (part, block) in deferred:
            skipped = jnp.logical_or(skipped, skips_z)
        if part in RING_FAR:
            skipped = jnp.logical_or(skipped, skips_far)
        return skipped


    def panel(steps):
        return lax.rem(here + steps + panels, panels)

    to_x = panel(1 - 2 * x)
    to_y = panel(2 * way)
    to_z = panel(4 * way)
    from_z = panel(-4 * way)
    to_start = panel(2)
    to_first = panel(3)

    locals_here = [
        pltpu.make_async_copy(
            local_ref.at[0, sub // SPLIT, pl.ds(part * piece + sub % SPLIT * small, small)],
            windows[part].at[OWN, sub],
            local_sem,
        )
        for part in range(PARTS)
        for sub in range(subs)
    ]
    for copy in locals_here:
        copy.start()
    scalar_copies = [
        pltpu.make_async_copy(source, target, scalar_sem.at[i])
        for i, (source, target) in enumerate([(pairs_hbm, pairs_ref), (send_hbm, send_ref)])
    ]
    for copy in scalar_copies:
        copy.start()
    weight_copies = [
        pltpu.make_async_copy(weights_ref.at[0, 0], weights, weight_sem)
    ]
    near_copy = pltpu.make_async_copy(near_ref, near, near_sem)
    incident_copy = pltpu.make_async_copy(incident_ref, incident, incident_sem)

    barrier = pltpu.get_barrier_semaphore()

    def greet(semaphore, **device):
        pl.semaphore_signal(
            semaphore, inc=1, device_id=device, device_id_type=pl.DeviceIdType.MESH
        )

    greet(barrier, panel=to_x)
    greet(barrier, panel=to_y)

    @pl.when(jnp.logical_not(end))
    def _():
        greet(barrier, panel=from_z)

    @pl.when(start)
    def _():
        greet(barrier, panel=panel(-2))

        @pl.when(feeds_near)
        def _():
            greet(barrier, panel=panel(-3))
            greet(barrier, panel=panel(-1))

    @pl.when(gives)
    def _():
        greet(barrier, panel=panel(1))

    for ahead in range(1, lags):
        greet(barrier, lag=lax.rem(lag + ahead, lags))
    pl.semaphore_wait(
        barrier,
        1
        + lags
        + jnp.where(takes, 1, 0).astype(jnp.int32)
        + jnp.where(
            waits_long, 0,
            jnp.where(end, jnp.where(feeds_near, 3, 2), jnp.where(skips_z, 2, 1)),
        ).astype(jnp.int32),
    )
    @pl.when(takes)
    def _():
        greet(give_sem, panel=panel(-1))

    pltpu.make_async_copy(local_ref.at[0], local_ref.at[0], local_sem).wait()

    pieces = [(part, sub) for part in range(PARTS) for sub in range(subs)]
    backward = pieces[::-1]

    alone = min(NEAR_BY_X, FAR_BY_X)
    each = PARTS * subs
    relayed_across = (PARTS - alone) * subs

    def arrival(target, part, block):
        if target == BESIDE:
            return part * subs + block
        if target == BEYOND:
            return each + part * subs + block
        if target == ACROSS:
            place = (part - alone) * subs + block if part >= alone else relayed_across
            return 2 * each + place
        if target == FOURTH:
            return 2 * each + relayed_across + 1 + part
        return 2 * each + relayed_across + 1 + PARTS + (part - FAR_BY_X) * subs + block

    def copy_of(source, target, link, part, block, device, lands=None):
        return pltpu.make_async_remote_copy(
            src_ref=windows[part].at[source, block],
            dst_ref=windows[part].at[target, block],
            send_sem=send_sem.at[link],
            recv_sem=recv_sem.at[arrival(target, part, block) if lands is None else lands],
            device_id={"panel": device},
            device_id_type=pl.DeviceIdType.MESH,
        )

    def by_x(part, block):
        return copy_of(OWN, ACROSS, 0, part, block, to_x)

    def by_y(part, block):
        return copy_of(OWN, BESIDE, 0, part, block, to_y)

    def by_z(part, block):
        return copy_of(BESIDE, BEYOND, 0, part, block, to_z)

    def fourth_by_x(part, block):
        return copy_of(jnp.where(feeds_near, BESIDE, BEYOND), FOURTH, 1, part, block, to_x)

    def fourth_by_y(part, block):
        if part < FAR_BY_X:
            return copy_of(ACROSS, FOURTH, 1, part, block, to_y)
        lands = jnp.where(
            feeds_near, arrival(FOURTH, part, block), arrival(TRANSIT, part, block)
        )
        return copy_of(
            ACROSS, jnp.where(feeds_near, FOURTH, TRANSIT), 1, part, block, to_y, lands
        )

    def fourth_by_z(part, block):
        return copy_of(TRANSIT, FOURTH, 1, part, block, to_z)

    def by_ring(part, block):
        return copy_of(OWN, BEYOND, 1, part, block, to_start)

    def fourth_by_ring(part, block):
        return copy_of(ACROSS, FOURTH, 1, part, block, to_start)

    def fourth_at_once(part, block):
        return copy_of(BESIDE, FOURTH, 1, part, block, to_first)

    def fourth_straight(part, block):
        return copy_of(OWN, FOURTH, 1, part, block, panel(1))

    def landing(slot, part, block):
        return copy_of(slot, slot, 0, part, block, to_x)

    def bulk(number, link, lands):
        rows = number * small * fields // (2 * weights.shape[2])
        stretch = weights.at[pl.ds(0, 2), pl.ds(0, rows)]
        return pltpu.make_async_remote_copy(
            src_ref=stretch, dst_ref=stretch,
            send_sem=send_sem.at[link], recv_sem=recv_sem.at[lands],
            device_id={"panel": to_x}, device_id_type=pl.DeviceIdType.MESH,
        )

    for one, other in zip(backward, pieces):
        by_y(*other).start()
        by_x(*one).start()
        if other[0] in RING:
            @pl.when(jnp.logical_and(end, feeds_near))
            def _():
                by_ring(*other).start()

        if other[0] in RING_FAR:
            @pl.when(jnp.logical_and(end, feeds_far))
            def _():
                by_ring(*other).start()

        if other[0] in STRAIGHT:
            @pl.when(jnp.logical_and(end, feeds_near))
            def _():
                fourth_straight(*other).start()

    for copy in weight_copies:
        copy.start()
    incident_copy.start()
    near_copy.start()

    def pass_greeting():
        @pl.when(jnp.logical_not(first))
        def _():
            pl.semaphore_wait(chain_sem, 1)

        @pl.when(jnp.logical_not(last))
        def _():
            greet(chain_sem, panel=to_z)

    @pl.when(jnp.logical_and(y == 1, at_chain <= 1))
    def _():
        pass_greeting()

    for copy in scalar_copies:
        copy.wait()
    live = counts_ref[0, 0]
    readers = running.shape[0]
    steps_of = (0, 1 - 2 * x, 2 * way, -2 * way, 2 * x - 1)
    chosen = []
    for steps in steps_of:
        row = []
        for slot in range(slots):
            index, found, reader = 0, 0, 0
            for k in range(count):
                hit = jnp.logical_and(
                    jnp.logical_and(
                        pairs_ref[0, 0, 0, k] == reach + steps, pairs_ref[0, 1, 0, k] == slot
                    ),
                    k < live,
                )
                index = jnp.where(hit, k, index)
                found = jnp.where(hit, 1, found)
                reader = jnp.where(hit, pairs_ref[0, 2, 0, k], reader)
            block = send_ref[0, reach + steps, slot, panel(steps)]
            row.append((index, found, reader, block))
        chosen.append(row)
    for copy in weight_copies:
        copy.wait()

    z_last = jnp.logical_and(start, feeds_near)
    lasting_place = (jnp.where(z_last, FOURTH, BEYOND), jnp.where(z_last, BEYOND, FOURTH))
    pairs_of = list(zip(chosen[FOURTH], chosen[BEYOND]))
    lasting = (
        [[jnp.where(z_last, f, b) for f, b in zip(*both)] for both in pairs_of],
        [[jnp.where(z_last, b, f) for f, b in zip(*both)] for both in pairs_of],
    )

    def block_of(part, place, b):
        return windows[part][place, b * SPLIT:(b + 1) * SPLIT].reshape((piece, fields))

    def product(terms, at, columns):
        left, right = [], []
        for place, part in terms:
            entries = chosen[place] if place < LASTING else lasting[place - LASTING]
            place = place if place < LASTING else lasting_place[place - LASTING]
            for index, found, reader, block in entries:
                left.append(weights[index, at, part * piece:(part + 1) * piece])
                value = block_of(part, place, 0)
                for b in range(1, blocks):
                    value = jnp.where(block == b, block_of(part, place, b), value)
                kept = [
                    jnp.where(
                        jnp.logical_and(found == 1, reader == r), value, jnp.zeros_like(value)
                    )
                    for r in columns
                ]
                right.append(jnp.concatenate(kept, axis=1))
        return jnp.dot(
            jnp.concatenate(left, axis=1), jnp.concatenate(right, axis=0),
            preferred_element_type=jnp.float32,
        )

    rows = depth // CHUNKS
    chunks = [slice(chunk * rows, (chunk + 1) * rows) for chunk in range(CHUNKS)]

    def add(*terms, fresh=False):
        for at in chunks:
            term = product(terms, at, range(readers))
            for r in range(readers):
                column = term[:, r * fields:(r + 1) * fields]
                running[r, at] = column if fresh else running[r, at] + column

    add(*[(OWN, part) for part in range(PARTS)], fresh=True)

    deferred = [(part, block) for part, block in pieces if part in AT_ONCE][:DEFERRED]

    for step in range(len(pieces) + max(ASIDE, BEHIND)):
        if step < len(pieces):
            part, block = pieces[step]

            @pl.when(end)
            def _():
                if backward[step][0] >= alone:
                    landing(ACROSS, *backward[step]).wait_recv()
                if backward[step][0] in HANDED:
                    @pl.when(feeds_far)
                    def _():
                        fourth_by_ring(*backward[step]).start()

            landing(BESIDE, part, block).wait_recv()
            if part in AT_ONCE:
                @pl.when(skips_z)
                def _():
                    fourth_at_once(part, block).start()

            if step < LATE_GREETING:
                @pl.when(jnp.logical_not(jnp.logical_or(waits_long, stays(part, block))))
                def _():
                    by_z(part, block).start()
            else:
                if step == LATE_GREETING:
                    @pl.when(waits_long)
                    def _():
                        pass_greeting()
                        for missed in pieces[:step]:
                            by_z(*missed).start()

                @pl.when(jnp.logical_not(stays(part, block)))
                def _():
                    by_z(part, block).start()

            if deferred and (part, block) == deferred[-1]:
                @pl.when(skips_z)
                def _():
                    for missed in deferred:
                        by_z(*missed).start()

            if step == GIVE_STEP:
                @pl.when(gives)
                def _():
                    pl.semaphore_wait(give_sem, 1)
                    for given in pieces:
                        if given[0] >= FAR_BY_X:
                            fourth_straight(*given).start()

            if step == RING_STEP:
                @pl.when(start_far)
                def _():
                    for ring_part, ring_block in pieces:
                        if ring_part in RING:
                            landing(BEYOND, ring_part, ring_block).wait_recv()
                            fourth_by_x(ring_part, ring_block).start()

            @pl.when(feeds_near if part < NEAR_BY_X else near_end)
            def _():
                fourth_by_x(part, block).start()

        if ASIDE <= step < len(pieces) + ASIDE:
            turn = step - ASIDE
            part, block = backward[turn]

            @pl.when(jnp.logical_not(end))
            def _():
                if part >= alone:
                    landing(ACROSS, part, block).wait_recv()
                if part >= NEAR_BY_X:
                    @pl.when(near_aside)
                    def _():
                        fourth_by_y(part, block).start()

                if part >= FAR_BY_X:
                    @pl.when(far_aside)
                    def _():
                        fourth_by_y(part, block).start()

            if turn % subs == subs - 1:
                add((BESIDE, turn // subs))
        if step == 2 * SPLIT - 1:
            @pl.when(jnp.logical_and(y == 1, jnp.logical_and(at_chain > 1, jnp.logical_not(last))))
            def _():
                pass_greeting()
        if BEHIND <= step < len(pieces) + BEHIND:
            part, block = pieces[step - BEHIND]

            @pl.when(jnp.logical_and(feeds_far, jnp.logical_not(first)))
            def _():
                landing(BEYOND, part, block).wait_recv()
                if part < FAR_BY_X:
                    fourth_by_x(part, block).start()

        if step == len(pieces) - 1:
            bulk(alone * subs, 0, arrival(ACROSS, 0, 0)).wait_recv()
            add(*[(ACROSS, part) for part in range(alone)])
        if step == len(pieces) + ASIDE - 1:
            add(*[(ACROSS, part) for part in range(alone, PARTS)])

    @pl.when(far_over)
    def _():
        for part, block in backward:
            if part >= FAR_BY_X:
                landing(TRANSIT, part, block).wait_recv()
                fourth_by_z(part, block).start()

    def arrive(place, part):
        if place >= LASTING:
            @pl.when(z_last if place == LASTING else jnp.logical_not(z_last))
            def _():
                arrive(FOURTH, part)

            @pl.when(z_last if place > LASTING else jnp.logical_not(z_last))
            def _():
                arrive(BEYOND, part)

            return
        if place == BEYOND:
            @pl.when(jnp.logical_or(feeds_near, end if part in RING else first))
            def _():
                for block in range(subs):
                    landing(place, part, block).wait_recv()

            if part < FAR_BY_X:
                @pl.when(jnp.logical_and(end, feeds_far))
                def _():
                    for block in range(subs):
                        fourth_by_x(part, block).start()
        else:
            bulk(subs, 0, arrival(FOURTH, part, 0)).wait_recv()

    order = [((BEYOND, 0), (BEYOND, 1))]
    order += [((FOURTH, part - 2), (BEYOND, part)) for part in range(2, PARTS - 1)]
    order += [((FOURTH, part),) for part in range(PARTS - 3, PARTS - 2)]
    order += [((FOURTH, PARTS - 2), (LASTING, PARTS - 1)), ((LASTING + 1, PARTS - 1),)]
    for group in order[:-1]:
        for place, part in group:
            arrive(place, part)
        add(*group)
    incident_copy.wait()
    near_copy.wait()
    arrive(*order[-1][0])
    sums = []
    for chunk, at in enumerate(chunks):
        for ahead in range(1, lags):
            other = lax.rem(lag + ahead, lags)
            for j in range(own):
                reader = other * own + j
                theirs[ahead - 1, j, at] = running[reader, at] + product(
                    order[-1], at, [reader]
                )
            copy = pltpu.make_async_remote_copy(
                src_ref=theirs.at[ahead - 1, :, pl.ds(chunk * rows, rows)],
                dst_ref=landed.at[ahead - 1, :, pl.ds(chunk * rows, rows)],
                send_sem=sum_send_sem.at[ahead - 1],
                recv_sem=sum_recv_sem.at[ahead - 1, chunk],
                device_id={"lag": other},
                device_id_type=pl.DeviceIdType.MESH,
            )
            copy.start()
            sums.append(copy)
    for at in chunks:
        for j in range(own):
            reader = lag * own + j
            mine[j, at] = incident[j, at].astype(jnp.float32) - (
                running[reader, at] + product(order[-1], at, [reader])
            )
    def parts_of(taken):
        return subs * len([part for part in range(PARTS) if taken(part)])

    def when(condition, number):
        return jnp.where(condition, number, 0).astype(jnp.int32)

    near_x, far_x = NEAR_BY_X * subs, FAR_BY_X * subs
    ringed = parts_of(lambda part: part in RING)
    ringed_far = parts_of(lambda part: part in RING_FAR)
    straight = parts_of(lambda part: part in STRAIGHT)
    at_once = parts_of(lambda part: part in AT_ONCE)
    handed = parts_of(lambda part: part in HANDED)
    extra = jnp.where(
        feeds_near,
        near_x
        + when(near_end, each - near_x)
        + when(near_aside, each - near_x)
        + when(far_over, each - far_x)
        + when(gives, each - far_x)
        + when(end, ringed + straight),
        when(jnp.logical_not(first), far_x)
        + when(far_aside, each - far_x)
        + when(end, far_x + ringed_far + handed)
        + when(start, ringed)
        + when(before_end, at_once),
    )

    kept_back = when(skips_z, ringed) + when(skips_far, ringed_far)
    for number in sorted({0, ringed, ringed_far}):
        @pl.when(kept_back == number)
        def _():
            bulk(3 * each - number, 0, 0).wait_send()

    for number in range(subs, 3 * each, subs):
        @pl.when(extra == number)
        def _():
            bulk(number, 1, 0).wait_send()

    solved = [None] * own
    for chunk, at in enumerate(chunks):
        for copy in sums[chunk * (lags - 1):(chunk + 1) * (lags - 1)]:
            copy.wait_recv()
        for j in range(own):
            remainder = mine[j, at]
            for ahead in range(1, lags):
                remainder = remainder - landed[ahead - 1, j, at]
            remainder = remainder.astype(jnp.bfloat16)
            term = jnp.dot(near[j, :, at], remainder, preferred_element_type=jnp.float32)
            solved[j] = term if chunk == 0 else solved[j] + term
    for j in range(own):
        out_ref[j] = solved[j].astype(out_ref.dtype)
    for ahead in range(1, lags):
        whole = theirs.at[ahead - 1]
        pltpu.make_async_remote_copy(
            src_ref=whole, dst_ref=whole,
            send_sem=sum_send_sem.at[ahead - 1], recv_sem=sum_recv_sem.at[ahead - 1, 0],
            device_id={"lag": lax.rem(lag + ahead, lags)},
            device_id_type=pl.DeviceIdType.MESH,
        ).wait_send()


def relayed(panels, lags, history, weights, pairs, counts, send_list, incident, near_inverse):
    readers, depth, fields = history.shape[1:]
    count = weights.shape[2]
    own = incident.shape[0]
    piece = depth // PARTS
    subs = readers * SPLIT
    arrivals = PARTS * (2 * subs + 1) + 1 + subs * (
        2 * PARTS - min(NEAR_BY_X, FAR_BY_X) - FAR_BY_X
    )
    in_hbm = pl.BlockSpec(memory_space=pltpu.HBM)
    dma = pltpu.SemaphoreType.DMA
    held = [
        pltpu.with_memory_space_constraint(operand, pltpu.HBM)
        for operand in (
            jnp.transpose(pairs, (0, 3, 1, 2)), jnp.transpose(send_list, (1, 2, 3, 0)),
            history, weights, incident, near_inverse,
        )
    ]
    return pl.pallas_call(
        functools.partial(relay_kernel, panels, lags),
        out_shape=pltpu.VMEM(incident.shape, jnp.bfloat16),
        in_specs=[pl.BlockSpec(memory_space=pltpu.SMEM)] + [in_hbm] * 6,
        out_specs=pl.BlockSpec(memory_space=pltpu.VMEM),
        scratch_shapes=[
            *[pltpu.SMEM(operand.shape, operand.dtype) for operand in held[:2]],
            dma((2,)),
            [pltpu.VMEM((TRANSIT + 1, subs, piece // SPLIT, fields), history.dtype)] * PARTS,
            pltpu.VMEM(weights.shape[2:], weights.dtype),
            pltpu.VMEM(near_inverse.shape, near_inverse.dtype),
            pltpu.VMEM(incident.shape, incident.dtype),
            pltpu.VMEM((readers, depth, fields), jnp.float32),
            pltpu.VMEM((lags - 1, own, depth, fields), jnp.float32),
            pltpu.VMEM((own, depth, fields), jnp.float32),
            pltpu.VMEM((lags - 1, own, depth, fields), jnp.float32),
            dma((2,)),
            dma((arrivals,)),
            dma,
            dma,
            dma,
            dma,
            dma((lags - 1,)),
            dma((lags - 1, CHUNKS)),
            pltpu.SemaphoreType.REGULAR,
            pltpu.SemaphoreType.REGULAR,
        ],
        compiler_params=pltpu.CompilerParams(
            collective_id=0, has_side_effects=True, vmem_limit_bytes=48 * 1024 * 1024
        ),
    )(counts, *held)


def step_kernel(
    relay, panels, lags,
    pairs_ref, counts_ref, send_ref, local_ref, weights_ref, incident_ref, near_ref,
    out_ref,
    windows, weights, near, incident, right, running, partial_value, landed,
    send_sem, recv_sem, local_sem, weight_sem, near_sem, incident_sem,
    sum_send_sem, sum_recv_sem,
):
    here = lax.axis_index("panel")
    lag = lax.axis_index("lag")
    offsets = send_ref.shape[1]
    reach = offsets // 2
    blocks, piece, fields = windows[0].shape[1:]
    depth = piece * PARTS
    count = weights.shape[0]
    own = incident.shape[0]
    side = 2 * lax.rem(here, 2) - 1

    def panel(steps):
        return lax.rem(here + steps + panels, panels)

    def rows_of(part):
        return pl.ds(part * piece, piece)

    def outgoing(steps, part):
        if relay:
            return windows[part].at[0]
        return local_ref.at[reach - steps, :, rows_of(part)]

    source_here = local_ref.at[0] if relay else local_ref.at[reach]
    locals_here = [
        pltpu.make_async_copy(
            source_here.at[:, rows_of(part)], windows[part].at[0], local_sem.at[part]
        )
        for part in range(PARTS)
    ]
    for copy in locals_here:
        copy.start()
    weight_copies = [
        pltpu.make_async_copy(weights_ref.at[0, 0, k], weights.at[k], weight_sem.at[k])
        for k in range(count)
    ]

    barrier = pltpu.get_barrier_semaphore()
    greeted = [-side, 2 * side, -2 * side] + ([] if relay else [side])
    for steps in greeted:
        pl.semaphore_signal(
            barrier, inc=1, device_id={"panel": panel(steps)},
            device_id_type=pl.DeviceIdType.MESH,
        )
    for ahead in range(1, lags):
        pl.semaphore_signal(
            barrier, inc=1, device_id={"lag": lax.rem(lag + ahead, lags)},
            device_id_type=pl.DeviceIdType.MESH,
        )
    pl.semaphore_wait(barrier, len(greeted) + lags - 1)
    for copy in locals_here:
        copy.wait()

    def send(source, slot, part, steps):
        copy = pltpu.make_async_remote_copy(
            src_ref=source,
            dst_ref=windows[part].at[slot],
            send_sem=send_sem.at[slot - 1, part],
            recv_sem=recv_sem.at[slot - 1, part],
            device_id={"panel": panel(steps)},
            device_id_type=pl.DeviceIdType.MESH,
        )
        copy.start()
        return copy

    first, second, partner, passed = [], [], [], []
    lead = PARTS // 2
    for step in range(PARTS + lead):
        if step < PARTS:
            first.append(send(outgoing(2 * side, step), 3, step, 2 * side))
            partner.append(send(outgoing(-side, step), 4, step, -side))
        if step >= lead:
            part = step - lead
            second.append(send(outgoing(-2 * side, part), 2, part, -2 * side))
    near_copy = pltpu.make_async_copy(near_ref, near, near_sem)
    incident_copy = pltpu.make_async_copy(incident_ref, incident, incident_sem)
    for copy in weight_copies:
        copy.start()
    incident_copy.start()
    near_copy.start()
    def pass_on(part):
        if relay:
            first[part].wait_recv()
            passed.append(send(windows[part].at[3], 1, part, -side))
        else:
            passed.append(send(outgoing(side, part), 1, part, side))

    for part in range(PARTS):
        pass_on(part)
    for copy in weight_copies:
        copy.wait()
    incident_copy.wait()
    near_copy.wait()

    live = counts_ref[0, 0]
    readers = right.shape[2] // fields
    chosen = []
    for k in range(count):
        offset = pairs_ref[0, 0, 0, k]
        slot = pairs_ref[0, 1, 0, k]
        reader = pairs_ref[0, 2, 0, k]
        if relay:
            block = send_ref[0, offset, slot, panel(offset - reach)]
        else:
            block = slot
        place = lax.rem((offset - reach) * side + offsets, offsets)
        chosen.append((place, block, reader))

    def arrive(part):
        if not relay:
            first[part].wait_recv()
        partner[part].wait_recv()
        second[part].wait_recv()
        passed[part].wait_recv()
        for k, (place, block, reader) in enumerate(chosen):
            value = windows[part][place, block]
            for r in range(readers):
                kept = jnp.logical_and(reader == r, k < live)
                right[part, k * piece:(k + 1) * piece, r * fields:(r + 1) * fields] = jnp.where(
                    kept, value, jnp.zeros_like(value)
                )

    def product(part, at):
        left = jnp.concatenate(
            [weights[k, at, part * piece:(part + 1) * piece] for k in range(count)], axis=1
        )
        return jnp.dot(left, right[part], preferred_element_type=jnp.float32)

    rows = depth // CHUNKS
    sums = []
    for part in range(PARTS - 1):
        arrive(part)
        for chunk in range(CHUNKS):
            at = slice(chunk * rows, (chunk + 1) * rows)
            term = product(part, at)
            running[at, :] = term if part == 0 else running[at, :] + term
    arrive(PARTS - 1)
    for chunk in range(CHUNKS):
        at = slice(chunk * rows, (chunk + 1) * rows)
        total = running[at, :] + product(PARTS - 1, at)
        for r in range(readers):
            partial_value[r, at, :] = total[:, r * fields:(r + 1) * fields]
        for ahead in range(1, lags):
            other = lax.rem(lag + ahead, lags)
            copy = pltpu.make_async_remote_copy(
                src_ref=partial_value.at[pl.ds(other * own, own), pl.ds(chunk * rows, rows)],
                dst_ref=landed.at[ahead - 1, :, pl.ds(chunk * rows, rows)],
                send_sem=sum_send_sem.at[ahead - 1, chunk],
                recv_sem=sum_recv_sem.at[ahead - 1, chunk],
                device_id={"lag": other},
                device_id_type=pl.DeviceIdType.MESH,
            )
            copy.start()
            sums.append(copy)
    for copy in first + partner + second + passed:
        copy.wait_send()
    for copy in sums:
        copy.wait_recv()
    for j in range(own):
        summed = partial_value[lag * own + j]
        for ahead in range(1, lags):
            summed = summed + landed[ahead - 1, j]
        remainder = (incident[j].astype(jnp.float32) - summed).astype(jnp.bfloat16)
        out_ref[j] = jnp.dot(
            near[j], remainder, preferred_element_type=jnp.float32
        ).astype(out_ref.dtype)
    for copy in sums:
        copy.wait_send()


def on_device(panels, lags, history, weights, pairs, counts, send_list, incident, near_inverse):
    readers, depth, fields = history.shape[1:]
    offsets, slots = send_list.shape[2:]
    assert offsets == 5 and panels % 2 == 0 and panels > offsets
    count = weights.shape[2]
    own = incident.shape[0]
    if readers <= slots and panels % 4 == 0 and panels > 8:
        return relayed(
            panels, lags, history, weights, pairs, counts, send_list, incident, near_inverse
        )
    relay = readers <= slots
    blocks = readers if relay else slots
    local = history
    if not relay:
        here = lax.axis_index("panel")
        mine = lax.dynamic_index_in_dim(send_list, here, 0, keepdims=False)[0]
        local = jnp.take(history[0], mine.reshape(-1), axis=0).reshape(
            (offsets, slots, depth, fields)
        )
    anywhere = pl.BlockSpec(memory_space=pl.ANY)
    scalars = pl.BlockSpec(memory_space=pltpu.SMEM)
    dma = pltpu.SemaphoreType.DMA
    return pl.pallas_call(
        functools.partial(step_kernel, relay, panels, lags),
        out_shape=jax.ShapeDtypeStruct(incident.shape, jnp.bfloat16),
        in_specs=[scalars] * 3 + [anywhere] * 4,
        out_specs=pl.BlockSpec(memory_space=pltpu.VMEM),
        scratch_shapes=[
            [pltpu.VMEM((offsets, blocks, depth // PARTS, fields), history.dtype)] * PARTS,
            pltpu.VMEM(weights.shape[2:], weights.dtype),
            pltpu.VMEM(near_inverse.shape, near_inverse.dtype),
            pltpu.VMEM(incident.shape, incident.dtype),
            pltpu.VMEM((PARTS, count * depth // PARTS, readers * fields), history.dtype),
            pltpu.VMEM((depth, readers * fields), jnp.float32),
            pltpu.VMEM((readers, depth, fields), jnp.float32),
            pltpu.VMEM((lags - 1, own, depth, fields), jnp.float32),
            dma((offsets - 1, PARTS)),
            dma((offsets - 1, PARTS)),
            dma((PARTS,)),
            dma((count,)),
            dma,
            dma,
            dma((lags - 1, CHUNKS)),
            dma((lags - 1, CHUNKS)),
        ],
        compiler_params=pltpu.CompilerParams(
            collective_id=0, has_side_effects=True, vmem_limit_bytes=67043328
        ),
    )(jnp.transpose(pairs, (0, 3, 1, 2)), counts, jnp.transpose(send_list, (1, 2, 3, 0)), local, weights, incident, near_inverse)


def solution(mesh):
    return jax.shard_map(
        functools.partial(on_device, mesh.shape["panel"], mesh.shape["lag"]),
        mesh=mesh,
        in_specs=(
            P("lag", "panel", None, None),
            P("panel", "lag", None, None, None),
            P("panel", "lag", None, None),
            P("panel", "lag"),
            P(None, "lag", None, None),
            P(("panel", "lag"), None, None),
            P(("panel", "lag"), None, None),
        ),
        out_specs=P(("panel", "lag"), None, None),
        check_vma=False,
    )
```
